128 devices in a mesh: op: 16 (over z_lo, y, core), tm: 8 (over x, z_hi).
Axes of the slice: x: 4, y: 4, z: 4 (z_hi: 2, z_lo: 2; z = z_hi * 2 + z_lo), core: 2. Of those that a mesh axis runs over, the one named last changes fastest.
Arguments:
- phi: bfloat16 [256, 64, 2, 128, 128], P('op', 'tm'), may hold values from -6 to 6
- tau_fwd: bfloat16 [2, 64, 2, 128, 128], P(None, 'tm'), may hold values from -0.375 to 0.375
- tau_bwd: bfloat16 [2, 64, 2, 128, 128], P(None, 'tm'), may hold values from -0.375 to 0.375
- src_times: int32 [2], replicated, may hold values from 0 to 63
- partner: int32 [256], replicated, may hold values from 0 to 255, each once
Outputs:
- corr: float32 [256, 2, 64, 2, 256], P('op', None, 'tm')
The draws below stay inside these ranges and needn't reach their ends.
Inputs may be any that keep to these rules, and one draw needn't show every extreme that they name: partner is a permutation of the operators. `src_times`: source times may repeat.
All inputs are finite; a program needn't handle non-finite values.
Results may differ from the reference program's by a relative error of at most 0.0041.
Values may be sent and summed in bfloat16 or wider, within the bound.
A program may use at most 256 MiB of HBM per device.

```python
import jax
import jax.numpy as jnp
from jax import lax

NV = 128
OPS = 256
NSRC = 2
NT = 64


def level_of(stream_key, shape, cuts, smallest, top_value):
    def one(dim, blocks):
        draws = jax.random.uniform(jax.random.fold_in(jax.random.fold_in(stream_key, 6), dim), (blocks,), jnp.float32, smallest / len(cuts), top_value / len(cuts))
        return jnp.repeat(jnp.exp(draws), shape[dim] // blocks).reshape((-1,) + (1,) * (len(shape) - dim - 1))

    gain = one(*cuts[0])
    for cut in cuts[1:]:
        gain = gain * one(*cut)
    return gain


def centred(rng, dims, scale, limit, pieces=(), kind=jnp.bfloat16):
    loudness = level_of(rng, dims, pieces, -0.22, 0.18) if pieces else 1.0
    values = jax.random.normal(rng, dims, jnp.float32) * scale * loudness
    return jnp.minimum(jnp.maximum(values, -limit), limit).astype(kind)


def setup_inputs(seed: int = 0) -> dict:
    keys = jax.random.split(jax.random.key(seed), 6)
    return {
        "phi": centred(keys[0], (OPS, NT, 2, NV, NV), 1.0, 6.0, ((0, 16), (1, 8))),
        "tau_fwd": centred(keys[1], (NSRC, NT, 2, NV, NV), (2 * NV) ** -0.5, 0.375, ((1, 8),)),
        "tau_bwd": centred(keys[2], (NSRC, NT, 2, NV, NV), (2 * NV) ** -0.5, 0.375, ((1, 8),)),
        "src_times": jax.random.randint(keys[3], (NSRC,), 0, NT).astype(jnp.int32),
        "partner": jax.random.permutation(keys[4], OPS).astype(jnp.int32),
    }


def rounded(value):
    low = lax.optimization_barrier(value.astype(jnp.bfloat16))
    return low.astype(jnp.float32)


def complex_product(spec, left_re, left_im, right_re, right_im):
    def inner(first, second):
        return jnp.einsum(spec, first, second)
    return inner(left_re, right_re) - inner(left_im, right_im), inner(left_re, right_im) + inner(left_im, right_re)


def reference(phi, tau_fwd, tau_bwd, src_times, partner):
    source = jnp.take(phi, src_times.astype(jnp.int32), axis=1).astype(jnp.float32)
    source_re = source[:, :, 0]
    source_im = source[:, :, 1]

    def one_time(when):
        fields = lax.dynamic_index_in_dim(phi, when, 1, False).astype(jnp.float32)
        fwd = lax.dynamic_index_in_dim(tau_fwd, when, 1, False).astype(jnp.float32)
        bwd = lax.dynamic_index_in_dim(tau_bwd, when, 1, False).astype(jnp.float32)
        left_re, left_im = complex_product("sab,jbc->jsac", fwd[:, 0], fwd[:, 1], fields[:, 0], fields[:, 1])
        left_re, left_im = rounded(left_re), rounded(left_im)
        sink_re, sink_im = complex_product("jsac,scd->jsad", left_re, left_im, bwd[:, 0], bwd[:, 1])
        sink_re, sink_im = rounded(sink_re), rounded(sink_im)
        real_part = jnp.einsum("jsad,ksad->jsk", sink_re, source_re) + jnp.einsum("jsad,ksad->jsk", sink_im, source_im)
        imag_part = jnp.einsum("jsad,ksad->jsk", sink_im, source_re) - jnp.einsum("jsad,ksad->jsk", sink_re, source_im)
        return jnp.stack([real_part, imag_part], 2) / NV

    result = lax.map(one_time, jnp.arange(NT, dtype=jnp.int32))
    result = jnp.transpose(result, (1, 2, 0, 3, 4))
    return jnp.take(result, partner.astype(jnp.int32), axis=4)
```

```python
import functools

import jax
import jax.numpy as jnp
from jax import lax
from jax.experimental import pallas as pl
from jax.experimental.pallas import tpu as pltpu
from jax.sharding import PartitionSpec as P

MESH = pl.DeviceIdType.MESH
F32 = jnp.float32
BF16 = jnp.bfloat16
NSEM = 136
COLORS = ((0, 22, "xyz"), (22, 42, "yzx"), (42, 64, "zxy"))


def nxt(v, step):
    return lax.rem(v + step, 4)


def kernel(src, cand, phi, tauf, taub, partner, out, S, P2, acc, stage, fbuf, fl, wb, rs, comb, dd,
           send_sem, recv_sem, phi_sem):
    op = lax.axis_index("op")
    tm = lax.axis_index("tm")
    core = lax.rem(op, 2)
    zl = op // 8
    zh = lax.rem(tm, 2)
    pos = {"x": tm // 2, "y": lax.rem(op // 2, 4), "z": 2 * zh + zl}

    def device(moved, other_core=False):
        at = dict(pos)
        at.update(moved)
        c = 1 - core if other_core else core
        return ((lax.rem(at["z"], 2) * 4 + at["y"]) * 2 + c, at["x"] * 2 + at["z"] // 2)

    count = [0]
    pending = []

    def send(src_ref, dst_ref, target):
        n = count[0]
        count[0] += 1
        copy = pltpu.make_async_remote_copy(
            src_ref=src_ref, dst_ref=dst_ref, send_sem=send_sem.at[n], recv_sem=recv_sem.at[n],
            device_id=target, device_id_type=MESH)
        copy.start()
        pending.append(copy)
        return copy

    def phi_copy(t):
        slot = lax.rem(t, 2)
        return pltpu.make_async_copy(phi.at[:, t], fbuf.at[slot], phi_sem.at[slot])

    phi_copy(0).start()

    peers = [device({d: nxt(pos[d], k)}) for d in "xyz" for k in (1, 3)]
    peers += [device({"z": nxt(pos["z"], 2)}), device({}, True)]
    barrier = pltpu.get_barrier_semaphore()
    for peer in peers:
        pl.semaphore_signal(barrier, inc=1, device_id=peer, device_id_type=MESH)
    pl.semaphore_wait(barrier, len(peers))

    def sandwich(t, carry):
        slot = lax.rem(t, 2)
        phi_copy(t).wait()

        @pl.when(t < 7)
        def _():
            phi_copy(t + 1).start()

        for s in range(2):
            fr, fi = tauf[s, t, 0], tauf[s, t, 1]
            fl[0:128, 0:128] = fr
            fl[0:128, 128:256] = -fi
            fl[128:256, 0:128] = fi
            fl[128:256, 128:256] = fr
            br, bi = taub[s, t, 0], taub[s, t, 1]
            wb[0:128, 0:128] = br
            wb[0:128, 128:256] = bi
            wb[128:256, 0:128] = -bi
            wb[128:256, 128:256] = br

            def pair(jp, c2):
                two = [fbuf[slot, 2 * jp + q].reshape(256, 128) for q in range(2)]
                a = jnp.dot(fl[...], jnp.concatenate(two, axis=1), preferred_element_type=F32).astype(BF16)
                for q in range(2):
                    left = jnp.concatenate([a[0:128, q * 128:q * 128 + 128], a[128:256, q * 128:q * 128 + 128]], axis=1)
                    prod = jnp.dot(left, wb[...], preferred_element_type=F32)
                    row = pl.multiple_of((2 * jp + q) * 128, 128)
                    stage[0, pl.ds(row, 128), :] = prod[:, 0:128]
                    stage[1, pl.ds(row, 128), :] = prod[:, 128:256]
                return c2

            lax.fori_loop(0, 8, pair, 0)

            def turn(ab, c2):
                for q in range(8):
                    for r in range(2):
                        a = ab * 8 + q
                        rows = stage[r, pl.ds(a, 16, stride=128), :]
                        P2[s, a, r, pl.ds(pl.multiple_of(t * 16, 16), 16), :] = rows.astype(BF16)
                return c2

            lax.fori_loop(0, 16, turn, 0)
        return carry

    own_tm = [src[s] // 8 for s in range(2)]
    own_x = [v // 2 for v in own_tm]
    own_zh = [lax.rem(v, 2) for v in own_tm]
    x = pos["x"]
    xp, xm, x2 = nxt(x, 1), nxt(x, 3), nxt(x, 2)
    plus, minus = device({"x": xp}), device({"x": xm})
    first = [
        send(cand.at[x2, 0], rs.at[0], plus),
        send(cand.at[x2, 1], rs.at[1], minus),
        send(cand.at[xp, 1], rs.at[2], plus),
        send(cand.at[xm, 0], rs.at[3], minus),
    ]
    lax.fori_loop(0, 4, sandwich, 0)
    first[0].wait_recv()
    first[1].wait_recv()
    for s in range(2):
        h = slice(32 * s, 32 * s + 32)
        comb[0, h] = jnp.where(own_x[s] == xm, rs[0, h], cand[xp, 0, h])
        comb[1, h] = jnp.where(own_x[s] == xp, rs[1, h], cand[xm, 1, h])
    second = [send(comb.at[0], rs.at[4], plus), send(comb.at[1], rs.at[5], minus)]
    lax.fori_loop(4, 6, sandwich, 0)
    for copy in first[2:] + second:
        copy.wait_recv()
    for s in range(2):
        h = slice(32 * s, 32 * s + 32)
        dd[0, h] = jnp.where(own_x[s] == x, cand[x, 0, h], jnp.where(own_x[s] == xp, rs[3, h], rs[4, h]))
        dd[1, h] = jnp.where(own_x[s] == x, cand[x, 1, h], jnp.where(own_x[s] == xm, rs[2, h], rs[5, h]))
    across = send(dd.at[1 - zh], rs.at[6], device({"z": nxt(pos["z"], 2)}))
    lax.fori_loop(6, 8, sandwich, 0)
    across.wait_recv()
    for s in range(2):
        h = slice(32 * s, 32 * s + 32)
        S[pos["x"], pos["z"], pos["y"], core, h] = jnp.where(own_zh[s] == zh, dd[zh, h], rs[6, h])

    whole = pl.ds(0, 4)

    def box(where, lo, hi):
        at = [where[d] for d in "xzy"]
        return S.at[at[0], at[1], at[2], pl.ds(core, 1), pl.ds(lo, hi - lo)]

    def one(v):
        return pl.ds(v, 1)

    mate = device({}, True)
    mate_copies = {0: [], 1: [], 2: []}

    def share(color, where, lo, hi):
        ref = box(where, lo, hi)
        mate_copies[color].append(send(ref, ref, mate))

    def ring1(color, d, where):
        lo, hi, _ = COLORS[color]
        w = dict(where)
        w[d] = one(pos[d])
        ref = box(w, lo, hi)
        return [send(ref, ref, device({d: nxt(pos[d], k)})) for k in (1, 3)]

    def ring2(color, d, where):
        lo, hi, _ = COLORS[color]
        mid = (lo + hi) // 2
        w = dict(where)
        w[d] = one(nxt(pos[d], 3))
        a = box(w, lo, mid)
        w[d] = one(nxt(pos[d], 1))
        b = box(w, mid, hi)
        return [send(a, a, device({d: nxt(pos[d], 1)})), send(b, b, device({d: nxt(pos[d], 3)}))]

    def arrived(copies):
        for copy in copies:
            copy.wait_recv()

    three = range(3)
    order = [COLORS[c][2] for c in three]
    base = {d: one(pos[d]) for d in "xyz"}
    p1 = [ring1(c, order[c][0], base) for c in three]
    p1b, p2, p2b = [None] * 3, [None] * 3, [None] * 3
    p3 = [[None] * 4 for _ in three]
    p3b = [[None] * 4 for _ in three]
    for c in three:
        arrived(p1[c])
        p1b[c] = ring2(c, order[c][0], base)
    line = [dict(base) for _ in three]
    for c in three:
        arrived(p1b[c])
        line[c][order[c][0]] = whole
        p2[c] = ring1(c, order[c][1], line[c])
        p3[c][0] = ring1(c, order[c][2], line[c])
        share(c, line[c], COLORS[c][0], COLORS[c][1])

    def group(c, k):
        w = dict(line[c])
        w[order[c][1]] = one(nxt(pos[order[c][1]], (0, 3, 1, 2)[k]))
        return w

    for c in three:
        arrived(p2[c])
        p2b[c] = ring2(c, order[c][1], line[c])
        for k in (1, 2):
            p3[c][k] = ring1(c, order[c][2], group(c, k))
            share(c, group(c, k), COLORS[c][0], COLORS[c][1])
    for c in three:
        arrived(p2b[c])
        p3[c][3] = ring1(c, order[c][2], group(c, 3))
        share(c, group(c, 3), COLORS[c][0], COLORS[c][1])
    for k in range(4):
        for c in three:
            arrived(p3[c][k])
            p3b[c][k] = ring2(c, order[c][2], group(c, k))
            for step in (3, 1):
                w = group(c, k)
                w[order[c][2]] = one(nxt(pos[order[c][2]], step))
                share(c, w, COLORS[c][0], COLORS[c][1])
    for k in range(4):
        for c in three:
            arrived(p3b[c][k])
            w = group(c, k)
            w[order[c][2]] = one(nxt(pos[order[c][2]], 2))
            share(c, w, COLORS[c][0], COLORS[c][1])

    acc[...] = jnp.zeros_like(acc)

    def contract(s, a0, a1):
        def step(p, c2):
            xx = p // 2
            z0 = lax.rem(p, 2) * 2
            left, right = [], []
            for a in range(a0, a1):
                half = [S[xx, pl.ds(z0, 2), :, :, s * 32 + a * 2 + r].reshape(256, 128) for r in range(2)]
                left.append(jnp.concatenate(half, axis=0))
                right.append(P2[s, p * 16 + a].reshape(256, 128))
            acc[s] += lax.dot_general(
                jnp.concatenate(left, axis=1), jnp.concatenate(right, axis=1),
                (((1,), (1,)), ((), ())), preferred_element_type=F32)
            return c2

        lax.fori_loop(0, 8, step, 0)

    parts = {0: ((0, 0, 11),), 1: ((0, 11, 16), (1, 0, 5)), 2: ((1, 5, 16),)}
    for c in three:
        arrived(mate_copies[c])
        for part in parts[c]:
            contract(*part)

    hot = (partner[...] == lax.broadcasted_iota(jnp.int32, (256, 256), 0)).astype(F32)
    for s in range(2):
        q = acc[s]
        real = q[0:256, 0:128] + q[256:512, 128:256]
        imag = q[0:256, 128:256] - q[256:512, 0:128]
        for r, v in enumerate((real, imag)):
            got = lax.dot_general(v, hot, (((0,), (0,)), ((), ())), precision=lax.Precision.HIGHEST,
                                  preferred_element_type=F32)
            out[s, r] = got * (1.0 / 128.0)
    for copy in pending:
        copy.wait_send()


def body(phi, tau_fwd, tau_bwd, src_times, partner):
    picked = jnp.stack([lax.dynamic_index_in_dim(phi, src_times[s] % 8, 1, False) for s in range(2)])
    cand = picked.reshape(2, 16, 2, 4, 2, 16, 128).transpose(3, 4, 0, 5, 2, 1, 6).reshape(4, 2, 64, 16, 128)
    vm = pl.BlockSpec(memory_space=pltpu.VMEM)
    res = pl.pallas_call(
        kernel,
        out_shape=jax.ShapeDtypeStruct((2, 2, 128, 256), F32),
        in_specs=[pl.BlockSpec(memory_space=pltpu.SMEM), vm, pl.BlockSpec(memory_space=pl.ANY), vm, vm, vm],
        out_specs=vm,
        scratch_shapes=[
            pltpu.VMEM((4, 4, 4, 2, 64, 16, 128), BF16),
            pltpu.VMEM((2, 128, 2, 128, 128), BF16),
            pltpu.VMEM((2, 512, 256), F32),
            pltpu.VMEM((2, 2048, 128), F32),
            pltpu.VMEM((2, 16, 2, 128, 128), BF16),
            pltpu.VMEM((256, 256), BF16),
            pltpu.VMEM((256, 256), BF16),
            pltpu.VMEM((7, 64, 16, 128), BF16),
            pltpu.VMEM((2, 64, 16, 128), BF16),
            pltpu.VMEM((2, 64, 16, 128), BF16),
            pltpu.SemaphoreType.DMA((NSEM,)),
            pltpu.SemaphoreType.DMA((NSEM,)),
            pltpu.SemaphoreType.DMA((2,)),
        ],
        compiler_params=pltpu.CompilerParams(collective_id=0, has_side_effects=True, vmem_limit_bytes=67043328),
    )(src_times, cand, phi, tau_fwd, tau_bwd, partner.reshape(1, 256))
    return res.reshape(2, 2, 8, 16, 256).transpose(3, 0, 2, 1, 4)


def solution(mesh):
    in_specs = (
        P("op", "tm", None, None, None),
        P(None, "tm", None, None, None),
        P(None, "tm", None, None, None),
        P(),
        P(),
    )
    out_specs = P("op", None, "tm", None, None)
    return jax.shard_map(body, mesh=mesh, in_specs=in_specs, out_specs=out_specs, check_vma=False)
```

```python
import functools

import jax
import jax.numpy as jnp
from jax import lax
from jax.experimental import pallas as pl
from jax.experimental.pallas import tpu as pltpu
from jax.sharding import PartitionSpec as P

MESH = pl.DeviceIdType.MESH
F32 = jnp.float32
BF16 = jnp.bfloat16
NSEM = 136
ROW = 132
COLORS = ((0, 22, "xyz"), (22, 42, "yzx"), (42, 64, "zxy"))


def nxt(v, step):
    return lax.rem(v + step, 4)


def kernel(src, phi, tauf_hbm, taub_hbm, partner, out, S, P2, acc, stage, abuf, fbuf, cand, tauf, taub, fl, wb, rs, comb, dd,
           send_sem, recv_sem, phi_sem, tau_sem, load_sem):
    op = lax.axis_index("op")
    tm = lax.axis_index("tm")
    core = lax.rem(op, 2)
    zl = op // 8
    zh = lax.rem(tm, 2)
    pos = {"x": tm // 2, "y": lax.rem(op // 2, 4), "z": 2 * zh + zl}

    def device(moved, other_core=False):
        at = dict(pos)
        at.update(moved)
        c = 1 - core if other_core else core
        return ((lax.rem(at["z"], 2) * 4 + at["y"]) * 2 + c, at["x"] * 2 + at["z"] // 2)

    count = [0]
    pending = []

    def send(src_ref, dst_ref, target):
        n = count[0]
        count[0] += 1
        copy = pltpu.make_async_remote_copy(
            src_ref=src_ref, dst_ref=dst_ref, send_sem=send_sem.at[n], recv_sem=recv_sem.at[n],
            device_id=target, device_id_type=MESH)
        copy.start()
        pending.append(copy)
        return copy

    def phi_copy(t):
        slot = lax.rem(t, 2)
        return pltpu.make_async_copy(phi.at[:, t], fbuf.at[slot], phi_sem.at[slot])

    loads = [pltpu.make_async_copy(phi.at[j], P2.at[0, j * 8:j * 8 + 8], load_sem.at[j]) for j in range(16)]
    for copy in loads:
        copy.start()
    peers = [device({d: nxt(pos[d], k)}) for d in "xyz" for k in (1, 3)]
    peers += [device({"z": nxt(pos["z"], 2)}), device({}, True)]
    barrier = pltpu.get_barrier_semaphore()
    for peer in peers:
        pl.semaphore_signal(barrier, inc=1, device_id=peer, device_id_type=MESH)
    taus = [pltpu.make_async_copy(tauf_hbm, tauf, tau_sem.at[0]), pltpu.make_async_copy(taub_hbm, taub, tau_sem.at[1])]
    for copy in taus:
        copy.start()
    phi_copy(0).start()

    for copy in loads:
        copy.wait()
    for s in range(2):
        when = lax.rem(src[s], 8)
        for j in range(16):
            for r in range(2):
                stage[r, j * ROW:j * ROW + 128, :] = P2[0, j * 8 + when, r].astype(F32)

        def deal(ab, c2):
            for q in range(8):
                for r in range(2):
                    rows = stage[r, pl.ds(ab * 8 + q, 16, stride=ROW), :]
                    cand[ab // 4, lax.rem(ab // 2, 2), s * 32 + lax.rem(ab, 2) * 16 + q * 2 + r] = rows.astype(BF16)
            return c2

        lax.fori_loop(0, 16, deal, 0)
    acc[...] = jnp.zeros_like(acc)
    for copy in taus:
        copy.wait()
    pl.semaphore_wait(barrier, len(peers))

    def sandwich(t, carry):
        slot = lax.rem(t, 2)
        phi_copy(t).wait()

        @pl.when(t < 7)
        def _():
            phi_copy(t + 1).start()

        for s in range(2):
            fr, fi = tauf[s, t, 0], tauf[s, t, 1]
            fl[0:128, 0:128] = fr
            fl[0:128, 128:256] = -fi
            fl[128:256, 0:128] = fi
            fl[128:256, 128:256] = fr
            br, bi = taub[s, t, 0], taub[s, t, 1]
            wb[0:128, 0:128] = br
            wb[0:128, 128:256] = bi
            wb[128:256, 0:128] = -bi
            wb[128:256, 128:256] = br

            for jp in range(8):
                two = [fbuf[slot, 2 * jp + q].reshape(256, 128) for q in range(2)]
                a = jnp.dot(fl[...], jnp.concatenate(two, axis=1), preferred_element_type=F32).astype(BF16)
                for q in range(2):
                    for r in range(2):
                        abuf[(2 * jp + q) * 128:(2 * jp + q) * 128 + 128, r * 128:r * 128 + 128] = a[r * 128:r * 128 + 128, q * 128:q * 128 + 128]
            for j in range(16):
                prod = jnp.dot(abuf[j * 128:j * 128 + 128, :], wb[...], preferred_element_type=F32)
                for r in range(2):
                    stage[r, j * ROW:j * ROW + 128, :] = prod[:, r * 128:r * 128 + 128]

            def turn(ab, c2):
                for q in range(8):
                    for r in range(2):
                        a = ab * 8 + q
                        rows = stage[r, pl.ds(a, 16, stride=ROW), :]
                        P2[s, a, r, pl.ds(pl.multiple_of(t * 16, 16), 16), :] = rows.astype(BF16)
                return c2

            lax.fori_loop(0, 16, turn, 0)
        return carry

    own_tm = [src[s] // 8 for s in range(2)]
    own_x = [v // 2 for v in own_tm]
    own_zh = [lax.rem(v, 2) for v in own_tm]
    x = pos["x"]
    xp, xm, x2 = nxt(x, 1), nxt(x, 3), nxt(x, 2)
    plus, minus = device({"x": xp}), device({"x": xm})
    first = [
        send(cand.at[x2, 0], rs.at[0], plus),
        send(cand.at[x2, 1], rs.at[1], minus),
        send(cand.at[xp, 1], rs.at[2], plus),
        send(cand.at[xm, 0], rs.at[3], minus),
    ]
    lax.fori_loop(0, 3, sandwich, 0)
    first[0].wait_recv()
    first[1].wait_recv()
    for s in range(2):
        h = slice(32 * s, 32 * s + 32)
        comb[0, h] = jnp.where(own_x[s] == xm, rs[0, h], cand[xp, 0, h])
        comb[1, h] = jnp.where(own_x[s] == xp, rs[1, h], cand[xm, 1, h])
    second = [send(comb.at[0], rs.at[4], plus), send(comb.at[1], rs.at[5], minus)]
    lax.fori_loop(3, 7, sandwich, 0)
    for copy in first[2:] + second:
        copy.wait_recv()
    for s in range(2):
        h = slice(32 * s, 32 * s + 32)
        dd[0, h] = jnp.where(own_x[s] == x, cand[x, 0, h], jnp.where(own_x[s] == xp, rs[3, h], rs[4, h]))
        dd[1, h] = jnp.where(own_x[s] == x, cand[x, 1, h], jnp.where(own_x[s] == xm, rs[2, h], rs[5, h]))
    across = send(dd.at[1 - zh], rs.at[6], device({"z": nxt(pos["z"], 2)}))
    lax.fori_loop(7, 8, sandwich, 0)
    across.wait_recv()
    for s in range(2):
        h = slice(32 * s, 32 * s + 32)
        S[pos["x"], pos["z"], pos["y"], core, h] = jnp.where(own_zh[s] == zh, dd[zh, h], rs[6, h])

    whole = pl.ds(0, 4)

    def box(where, lo, hi):
        at = [where[d] for d in "xzy"]
        return S.at[at[0], at[1], at[2], pl.ds(core, 1), pl.ds(lo, hi - lo)]

    def one(v):
        return pl.ds(v, 1)

    mate = device({}, True)
    mate_copies = {(c, k): [] for c in range(3) for k in range(4)}

    def share(color, k, where):
        ref = box(where, *COLORS[color][:2])
        mate_copies[color, k].append(send(ref, ref, mate))

    def ring1(color, d, where):
        lo, hi, _ = COLORS[color]
        w = dict(where)
        w[d] = one(pos[d])
        ref = box(w, lo, hi)
        return [send(ref, ref, device({d: nxt(pos[d], k)})) for k in (1, 3)]

    def ring2(color, d, where):
        lo, hi, _ = COLORS[color]
        mid = (lo + hi) // 2
        w = dict(where)
        w[d] = one(nxt(pos[d], 3))
        a = box(w, lo, mid)
        w[d] = one(nxt(pos[d], 1))
        b = box(w, mid, hi)
        return [send(a, a, device({d: nxt(pos[d], 1)})), send(b, b, device({d: nxt(pos[d], 3)}))]

    def arrived(copies):
        for copy in copies:
            copy.wait_recv()

    three = range(3)
    order = [COLORS[c][2] for c in three]
    base = {d: one(pos[d]) for d in "xyz"}
    p1 = [ring1(c, order[c][0], base) for c in three]
    p1b, p2, p2b = [None] * 3, [None] * 3, [None] * 3
    p3 = [[None] * 4 for _ in three]
    p3b = [[None] * 4 for _ in three]
    for c in three:
        arrived(p1[c])
        p1b[c] = ring2(c, order[c][0], base)
    line = [dict(base) for _ in three]
    for c in three:
        arrived(p1b[c])
        line[c][order[c][0]] = whole
        p2[c] = ring1(c, order[c][1], line[c])
        p3[c][0] = ring1(c, order[c][2], line[c])
        share(c, 0, line[c])

    def group(c, k):
        w = dict(line[c])
        w[order[c][1]] = one(nxt(pos[order[c][1]], (0, 3, 1, 2)[k]))
        return w

    for c in three:
        arrived(p2[c])
        p2b[c] = ring2(c, order[c][1], line[c])
        for k in (1, 2):
            p3[c][k] = ring1(c, order[c][2], group(c, k))
            share(c, k, group(c, k))
    for c in three:
        arrived(p2b[c])
        p3[c][3] = ring1(c, order[c][2], group(c, 3))
        share(c, 3, group(c, 3))
    def forward(k):
        for c in three:
            arrived(p3[c][k])
            p3b[c][k] = ring2(c, order[c][2], group(c, k))
            for step in (3, 1):
                w = group(c, k)
                w[order[c][2]] = one(nxt(pos[order[c][2]], step))
                share(c, k, w)

    def settle(k):
        for c in three:
            arrived(p3b[c][k])
            w = group(c, k)
            w[order[c][2]] = one(nxt(pos[order[c][2]], 2))
            share(c, k, w)

    def product(s, p, a0, a1, fields):
        left, right = [], []
        for a in range(a0, a1):
            half = [fields(s * 32 + a * 2 + r) for r in range(2)]
            left.append(jnp.concatenate(half, axis=0))
            right.append(P2[s, p * 16 + a].reshape(256, 128))
        return lax.dot_general(
            jnp.concatenate(left, axis=1), jnp.concatenate(right, axis=1),
            (((1,), (1,)), ((), ())), preferred_element_type=F32)

    def contract(k):
        for c in three:
            arrived(mate_copies[c, k])
            v = nxt(pos[order[c][1]], (0, 3, 1, 2)[k])
            if c == 0:
                def step(p, c2):
                    got = product(0, p, 0, 11, lambda slab: S[
                        p // 2, pl.ds(lax.rem(p, 2) * 2, 2), v, :, slab].reshape(64, 128))
                    acc[0, :, :, v] += got.reshape(2, 2, 32, 256)
                    return c2
                lax.fori_loop(0, 8, step, 0)
            elif c == 1:
                def step(xx, c2):
                    for s, a0, a1 in ((0, 11, 16), (1, 0, 5)):
                        got = product(s, xx * 2 + v // 2, a0, a1, lambda slab: S[xx, v, :, :, slab].reshape(128, 128))
                        acc[s, :, lax.rem(v, 2)] += got.reshape(2, 4, 32, 256)
                    return c2
                lax.fori_loop(0, 4, step, 0)
            else:
                def step(h, c2):
                    got = product(1, v * 2 + h, 5, 16, lambda slab: S[v, pl.ds(h * 2, 2), :, :, slab].reshape(256, 128))
                    acc[1] += got.reshape(2, 2, 4, 32, 256)
                    return c2
                lax.fori_loop(0, 2, step, 0)

    forward(0)
    forward(1)
    settle(0)
    forward(2)
    contract(0)
    settle(1)
    forward(3)
    contract(1)
    settle(2)
    settle(3)
    contract(2)
    contract(3)

    hot = (partner[...] == lax.broadcasted_iota(jnp.int32, (256, 256), 0)).astype(F32)
    for s in range(2):
        q = acc[s].reshape(512, 256)
        real = q[0:256, 0:128] + q[256:512, 128:256]
        imag = q[0:256, 128:256] - q[256:512, 0:128]
        for r, v in enumerate((real, imag)):
            got = lax.dot_general(v, hot, (((0,), (0,)), ((), ())), precision=lax.Precision.HIGHEST,
                                  preferred_element_type=F32)
            out[s, r] = got * (1.0 / 128.0)
    for copy in pending:
        copy.wait_send()


def body(phi, tau_fwd, tau_bwd, src_times, partner):
    vm = pl.BlockSpec(memory_space=pltpu.VMEM)
    hbm = pl.BlockSpec(memory_space=pl.ANY)
    res = pl.pallas_call(
        kernel,
        out_shape=jax.ShapeDtypeStruct((2, 2, 128, 256), F32),
        in_specs=[pl.BlockSpec(memory_space=pltpu.SMEM), hbm, hbm, hbm, vm],
        out_specs=vm,
        scratch_shapes=[
            pltpu.VMEM((4, 4, 4, 2, 64, 16, 128), BF16),
            pltpu.VMEM((2, 128, 2, 128, 128), BF16),
            pltpu.VMEM((2, 2, 2, 4, 32, 256), F32),
            pltpu.VMEM((2, 16 * ROW, 128), F32),
            pltpu.VMEM((2048, 256), BF16),
            pltpu.VMEM((2, 16, 2, 128, 128), BF16),
            pltpu.VMEM((4, 2, 64, 16, 128), BF16),
            pltpu.VMEM((2, 8, 2, 128, 128), BF16),
            pltpu.VMEM((2, 8, 2, 128, 128), BF16),
            pltpu.VMEM((256, 256), BF16),
            pltpu.VMEM((256, 256), BF16),
            pltpu.VMEM((7, 64, 16, 128), BF16),
            pltpu.VMEM((2, 64, 16, 128), BF16),
            pltpu.VMEM((2, 64, 16, 128), BF16),
            pltpu.SemaphoreType.DMA((NSEM,)),
            pltpu.SemaphoreType.DMA((NSEM,)),
            pltpu.SemaphoreType.DMA((2,)),
            pltpu.SemaphoreType.DMA((2,)),
            pltpu.SemaphoreType.DMA((16,)),
        ],
        compiler_params=pltpu.CompilerParams(collective_id=0, has_side_effects=True, vmem_limit_bytes=67043328),
    )(src_times, phi, tau_fwd, tau_bwd, partner.reshape(1, 256))
    return res.reshape(2, 2, 8, 16, 256).transpose(3, 0, 2, 1, 4)


def solution(mesh):
    in_specs = (
        P("op", "tm", None, None, None),
        P(None, "tm", None, None, None),
        P(None, "tm", None, None, None),
        P(),
        P(),
    )
    out_specs = P("op", None, "tm", None, None)
    return jax.shard_map(body, mesh=mesh, in_specs=in_specs, out_specs=out_specs, check_vma=False)
```

```python
import functools

import jax
import jax.numpy as jnp
from jax import lax
from jax.experimental import pallas as pl
from jax.experimental.pallas import tpu as pltpu
from jax.sharding import PartitionSpec as P

MESH = pl.DeviceIdType.MESH
F32 = jnp.float32
BF16 = jnp.bfloat16
NSEM = 168
ROW = 132
COLORS = ((0, 22, "xyz"), (22, 42, "yzx"), (42, 64, "zxy"))
PARTS = (((0, 0, 6), (1, 0, 5)), ((0, 6, 11), (1, 5, 10)), ((0, 11, 16), (1, 10, 16)))
GROUPS = ((0, 0, 4), (3, 0, 4), (1, 0, 4), (2, 0, 2), (2, 2, 2))
XF = 10
ZF = 16 - XF
ZH = ZF // 2


def nxt(v, step):
    return lax.rem(v + step, 4)


def kernel(src, phi, tauf_hbm, taub_hbm, partner, out, S, P2, acc, stage, abuf, fbuf, cand, tauf, taub, fl, wb, rs, comb, dd, rz, rw, ee, rv, comb2,
           send_sem, recv_sem, phi_sem, tau_sem, load_sem):
    op = lax.axis_index("op")
    tm = lax.axis_index("tm")
    core = lax.rem(op, 2)
    zl = op // 8
    zh = lax.rem(tm, 2)
    pos = {"x": tm // 2, "y": lax.rem(op // 2, 4), "z": 2 * zh + zl}

    def device(moved, other_core=False):
        at = dict(pos)
        at.update(moved)
        c = 1 - core if other_core else core
        return ((lax.rem(at["z"], 2) * 4 + at["y"]) * 2 + c, at["x"] * 2 + at["z"] // 2)

    count = [0]
    pending = []

    def send(src_ref, dst_ref, target):
        n = count[0]
        count[0] += 1
        copy = pltpu.make_async_remote_copy(
            src_ref=src_ref, dst_ref=dst_ref, send_sem=send_sem.at[n], recv_sem=recv_sem.at[n],
            device_id=target, device_id_type=MESH)
        copy.start()
        pending.append(copy)
        return copy

    def phi_copy(t):
        slot = lax.rem(t, 2)
        return pltpu.make_async_copy(phi.at[:, t], fbuf.at[slot], phi_sem.at[slot])

    loads = [pltpu.make_async_copy(phi.at[j], P2.at[0, j * 8:j * 8 + 8], load_sem.at[j]) for j in range(16)]
    for copy in loads:
        copy.start()
    peers = [device({d: nxt(pos[d], k)}) for d in "xyz" for k in (1, 3)]
    peers += [device({"z": nxt(pos["z"], 2)}), device({}, True)]
    barrier = pltpu.get_barrier_semaphore()
    for peer in peers:
        pl.semaphore_signal(barrier, inc=1, device_id=peer, device_id_type=MESH)
    taus = [pltpu.make_async_copy(tauf_hbm, tauf, tau_sem.at[0]), pltpu.make_async_copy(taub_hbm, taub, tau_sem.at[1])]
    for copy in taus:
        copy.start()
    phi_copy(0).start()

    for copy in loads:
        copy.wait()
    for s in range(2):
        when = lax.rem(src[s], 8)
        for j in range(16):
            for r in range(2):
                stage[r, j * ROW:j * ROW + 128, :] = P2[0, j * 8 + when, r].astype(F32)

        def deal(ab, c2):
            for q in range(8):
                for r in range(2):
                    rows = stage[r, pl.ds(ab * 8 + q, 16, stride=ROW), :]
                    cand[ab // 4, lax.rem(ab // 2, 2), lax.rem(ab, 2) * 8 + q, s * 2 + r] = rows.astype(BF16)
            return c2

        lax.fori_loop(0, 16, deal, 0)
    acc[...] = jnp.zeros_like(acc)
    for copy in taus:
        copy.wait()
    pl.semaphore_wait(barrier, len(peers))

    def sandwich(t, carry):
        slot = lax.rem(t, 2)
        phi_copy(t).wait()

        @pl.when(t < 7)
        def _():
            phi_copy(t + 1).start()

        for s in range(2):
            fr, fi = tauf[s, t, 0], tauf[s, t, 1]
            fl[0:128, 0:128] = fr
            fl[0:128, 128:256] = -fi
            fl[128:256, 0:128] = fi
            fl[128:256, 128:256] = fr
            br, bi = taub[s, t, 0], taub[s, t, 1]
            wb[0:128, 0:128] = br
            wb[0:128, 128:256] = bi
            wb[128:256, 0:128] = -bi
            wb[128:256, 128:256] = br

            for jp in range(8):
                two = [fbuf[slot, 2 * jp + q].reshape(256, 128) for q in range(2)]
                a = jnp.dot(fl[...], jnp.concatenate(two, axis=1), preferred_element_type=F32).astype(BF16)
                for q in range(2):
                    for r in range(2):
                        abuf[(2 * jp + q) * 128:(2 * jp + q) * 128 + 128, r * 128:r * 128 + 128] = a[r * 128:r * 128 + 128, q * 128:q * 128 + 128]
            for j in range(16):
                prod = jnp.dot(abuf[j * 128:j * 128 + 128, :], wb[...], preferred_element_type=F32)
                for r in range(2):
                    stage[r, j * ROW:j * ROW + 128, :] = prod[:, r * 128:r * 128 + 128]

            def turn(ab, c2):
                for q in range(8):
                    for r in range(2):
                        a = ab * 8 + q
                        rows = stage[r, pl.ds(a, 16, stride=ROW), :]
                        P2[s, a, r, pl.ds(pl.multiple_of(t * 16, 16), 16), :] = rows.astype(BF16)
                return c2

            lax.fori_loop(0, 16, turn, 0)
        return carry

    own_tm = [src[s] // 8 for s in range(2)]
    own_x = [v // 2 for v in own_tm]
    own_zh = [lax.rem(v, 2) for v in own_tm]
    x = pos["x"]
    xp, xm, x2 = nxt(x, 1), nxt(x, 3), nxt(x, 2)
    plus, minus = device({"x": xp}), device({"x": xm})
    far = device({"z": nxt(pos["z"], 2)})

    def choose(s, picks, last):
        value = last
        for condition, other in reversed(picks):
            value = jnp.where(condition[s], other, value)
        return value

    def pick(out_ref, pairs, last):
        for s in range(2):
            h = slice(2 * s, 2 * s + 2)
            out_ref[:, h] = choose(s, [(c, r[:, h]) for c, r in pairs], last[:, h])

    at_x = [v == x for v in own_x]
    at_xp = [v == xp for v in own_x]
    at_xm = [v == xm for v in own_x]
    at_zh = [v == zh for v in own_zh]

    early = pl.ds(0, XF)
    late = pl.ds(XF, ZF)
    pair1 = send(cand.at[:, 1 - zh, late], rz, far)
    first = [
        send(cand.at[x2, 0, early], rs.at[0], plus),
        send(cand.at[x2, 1, early], rs.at[1], minus),
        send(cand.at[xp, 1, early], rs.at[2], plus),
        send(cand.at[xm, 0, early], rs.at[3], minus),
    ]
    lax.fori_loop(0, 2, sandwich, 0)
    first[0].wait_recv()
    first[1].wait_recv()
    pick(comb.at[0], [(at_xm, rs.at[0])], cand.at[xp, 0, early])
    pick(comb.at[1], [(at_xp, rs.at[1])], cand.at[xm, 1, early])
    second = [send(comb.at[0], rs.at[4], plus), send(comb.at[1], rs.at[5], minus)]
    lax.fori_loop(2, 4, sandwich, 0)
    pair1.wait_recv()
    for q in range(4):
        pick(ee.at[q], [(at_zh, cand.at[q, zh, late])], rz.at[q])
    lo, hi = pl.ds(0, ZH), pl.ds(ZH, ZH)
    third = [
        send(ee.at[x2, lo], rv.at[0], plus),
        send(ee.at[x2, hi], rv.at[1], minus),
        send(ee.at[xp, hi], rv.at[2], plus),
        send(ee.at[xm, lo], rv.at[3], minus),
    ]
    for copy in first[2:] + second:
        copy.wait_recv()
    pick(dd.at[0], [(at_x, cand.at[x, 0, early]), (at_xp, rs.at[3])], rs.at[4])
    pick(dd.at[1], [(at_x, cand.at[x, 1, early]), (at_xm, rs.at[2])], rs.at[5])
    pair2 = send(dd.at[1 - zh], rw, far)
    lax.fori_loop(4, 5, sandwich, 0)
    third[0].wait_recv()
    third[1].wait_recv()
    pick(comb2.at[0], [(at_xm, rv.at[0])], ee.at[xp, lo])
    pick(comb2.at[1], [(at_xp, rv.at[1])], ee.at[xm, hi])
    fourth = [send(comb2.at[0], rv.at[4], plus), send(comb2.at[1], rv.at[5], minus)]
    lax.fori_loop(5, 6, sandwich, 0)
    own = S.at[pos["x"], pos["z"], pos["y"], core]
    pair2.wait_recv()
    for a in range(XF):
        for s in range(2):
            h = slice(2 * s, 2 * s + 2)
            own[4 * a + 2 * s:4 * a + 2 * s + 2] = choose(s, [(at_zh, dd[zh, a, h])], rw[a, h])
    for copy in third[2:] + fourth:
        copy.wait_recv()
    for half, mid, side, relay in ((0, at_xp, 3, 4), (1, at_xm, 2, 5)):
        for b in range(ZH):
            a = half * ZH + b
            for s in range(2):
                h = slice(2 * s, 2 * s + 2)
                row = 4 * (XF + a) + 2 * s
                own[row:row + 2] = choose(s, [(at_x, ee[x, a, h]), (mid, rv[side, b, h])], rv[relay, b, h])

    whole = pl.ds(0, 4)

    def box(where, lo, hi):
        at = [where[d] for d in "xzy"]
        return S.at[at[0], at[1], at[2], pl.ds(core, 1), pl.ds(lo, hi - lo)]

    def one(v):
        return pl.ds(v, 1)

    mate = device({}, True)
    mate_copies = {(c, k): [] for c in range(3) for k in range(len(GROUPS))}

    def share(color, k, where):
        ref = box(where, *COLORS[color][:2])
        mate_copies[color, k].append(send(ref, ref, mate))

    def ring1(color, d, where):
        lo, hi, _ = COLORS[color]
        w = dict(where)
        w[d] = one(pos[d])
        ref = box(w, lo, hi)
        return [send(ref, ref, device({d: nxt(pos[d], k)})) for k in (1, 3)]

    def ring2(color, d, where):
        lo, hi, _ = COLORS[color]
        mid = (lo + hi) // 2
        w = dict(where)
        w[d] = one(nxt(pos[d], 3))
        a = box(w, lo, mid)
        w[d] = one(nxt(pos[d], 1))
        b = box(w, mid, hi)
        return [send(a, a, device({d: nxt(pos[d], 1)})), send(b, b, device({d: nxt(pos[d], 3)}))]

    def arrived(copies):
        for copy in copies:
            copy.wait_recv()

    three = range(3)
    order = [COLORS[c][2] for c in three]
    base = {d: one(pos[d]) for d in "xyz"}
    p1 = [ring1(c, order[c][0], base) for c in three]
    p1b, p2, p2b = [None] * 3, [None] * 3, [None] * 3
    p3 = [[None] * len(GROUPS) for _ in three]
    p3b = [[None] * len(GROUPS) for _ in three]
    for c in three:
        arrived(p1[c])
        p1b[c] = ring2(c, order[c][0], base)
    line = [dict(base) for _ in three]
    for c in three:
        arrived(p1b[c])
        line[c][order[c][0]] = whole
        p2[c] = ring1(c, order[c][1], line[c])

    def group(c, k):
        step, first_place, places = GROUPS[k]
        w = dict(line[c])
        w[order[c][0]] = pl.ds(first_place, places)
        w[order[c][1]] = one(nxt(pos[order[c][1]], step))
        return w

    def spread(c, k):
        p3[c][k] = ring1(c, order[c][2], group(c, k))
        share(c, k, group(c, k))

    for c in three:
        spread(c, 0)
    lax.fori_loop(6, 8, sandwich, 0)
    for c in three:
        arrived(p2[c])
        p2b[c] = ring2(c, order[c][1], line[c])

    def forward(k):
        for c in three:
            arrived(p3[c][k])
            p3b[c][k] = ring2(c, order[c][2], group(c, k))
            for step in (3, 1):
                w = group(c, k)
                w[order[c][2]] = one(nxt(pos[order[c][2]], step))
                share(c, k, w)

    def settle(k):
        for c in three:
            arrived(p3b[c][k])
            w = group(c, k)
            w[order[c][2]] = one(nxt(pos[order[c][2]], 2))
            share(c, k, w)

    def product(s, p, a0, a1, fields):
        left, right = [], []
        for a in range(a0, a1):
            half = [fields(a * 4 + s * 2 + r) for r in range(2)]
            left.append(jnp.concatenate(half, axis=0))
            right.append(P2[s, p * 16 + a].reshape(256, 128))
        return lax.dot_general(
            jnp.concatenate(left, axis=1), jnp.concatenate(right, axis=1),
            (((1,), (1,)), ((), ())), preferred_element_type=F32)

    def contract(c, k):
        arrived(mate_copies[c, k])
        off, first_place, places = GROUPS[k]
        v = nxt(pos[order[c][1]], off)
        if c == 0:
            def step(p, c2):
                got = [product(*part[:1], p, *part[1:], lambda slab: S[
                    p // 2, pl.ds(lax.rem(p, 2) * 2, 2), v, :, slab].reshape(64, 128)) for part in PARTS[c]]
                for s, value in enumerate(got):
                    acc[s, :, :, v] += value.reshape(2, 2, 32, 256)
                return c2
            lax.fori_loop(2 * first_place, 2 * (first_place + places), step, 0, unroll=2)
        elif c == 1:
            ys = pl.ds(first_place, places)

            def step(xx, c2):
                got = [product(*part[:1], xx * 2 + v // 2, *part[1:], lambda slab: S[
                    xx, v, ys, :, slab].reshape(places * 32, 128)) for part in PARTS[c]]
                for s, value in enumerate(got):
                    acc[s, :, lax.rem(v, 2), ys] += value.reshape(2, places, 32, 256)
                return c2
            lax.fori_loop(0, 4, step, 0, unroll=2)
        else:
            for h in range(first_place // 2, (first_place + places) // 2):
                for part in PARTS[c]:
                    got = product(*part[:1], v * 2 + h, *part[1:], lambda slab: S[
                        v, 2 * h:2 * h + 2, :, :, slab].reshape(256, 128))
                    acc[part[0]] += got.reshape(2, 2, 4, 32, 256)

    def contract_all(k):
        for c in three:
            contract(c, k)

    def spread_all(k):
        for c in three:
            spread(c, k)

    forward(0)
    spread_all(1)
    spread_all(2)
    for c in three:
        arrived(p2b[c])
    settle(0)
    contract_all(0)
    forward(1)
    spread_all(3)
    forward(2)
    spread_all(4)
    settle(1)
    contract_all(1)
    forward(3)
    settle(2)
    forward(4)
    contract_all(2)
    settle(3)
    contract_all(3)
    settle(4)
    contract_all(4)

    hot = (partner[...] == lax.broadcasted_iota(jnp.int32, (256, 256), 0)).astype(F32)
    for s in range(2):
        q = acc[s].reshape(512, 256)
        real = q[0:256, 0:128] + q[256:512, 128:256]
        imag = q[0:256, 128:256] - q[256:512, 0:128]
        for r, v in enumerate((real, imag)):
            got = lax.dot_general(v, hot, (((0,), (0,)), ((), ())), precision=lax.Precision.HIGHEST,
                                  preferred_element_type=F32)
            out[s, r] = got * (1.0 / 128.0)
    for copy in pending:
        copy.wait_send()


def body(phi, tau_fwd, tau_bwd, src_times, partner):
    vm = pl.BlockSpec(memory_space=pltpu.VMEM)
    hbm = pl.BlockSpec(memory_space=pl.ANY)
    res = pl.pallas_call(
        kernel,
        out_shape=jax.ShapeDtypeStruct((2, 2, 128, 256), F32),
        in_specs=[pl.BlockSpec(memory_space=pltpu.SMEM), hbm, hbm, hbm, vm],
        out_specs=vm,
        scratch_shapes=[
            pltpu.VMEM((4, 4, 4, 2, 64, 16, 128), BF16),
            pltpu.VMEM((2, 128, 2, 128, 128), BF16),
            pltpu.VMEM((2, 2, 2, 4, 32, 256), F32),
            pltpu.VMEM((2, 16 * ROW, 128), F32),
            pltpu.VMEM((2048, 256), BF16),
            pltpu.VMEM((2, 16, 2, 128, 128), BF16),
            pltpu.VMEM((4, 2, 16, 4, 16, 128), BF16),
            pltpu.VMEM((2, 8, 2, 128, 128), BF16),
            pltpu.VMEM((2, 8, 2, 128, 128), BF16),
            pltpu.VMEM((256, 256), BF16),
            pltpu.VMEM((256, 256), BF16),
            pltpu.VMEM((6, XF, 4, 16, 128), BF16),
            pltpu.VMEM((2, XF, 4, 16, 128), BF16),
            pltpu.VMEM((2, XF, 4, 16, 128), BF16),
            pltpu.VMEM((4, ZF, 4, 16, 128), BF16),
            pltpu.VMEM((XF, 4, 16, 128), BF16),
            pltpu.VMEM((4, ZF, 4, 16, 128), BF16),
            pltpu.VMEM((6, ZH, 4, 16, 128), BF16),
            pltpu.VMEM((2, ZH, 4, 16, 128), BF16),
            pltpu.SemaphoreType.DMA((NSEM,)),
            pltpu.SemaphoreType.DMA((NSEM,)),
            pltpu.SemaphoreType.DMA((2,)),
            pltpu.SemaphoreType.DMA((2,)),
            pltpu.SemaphoreType.DMA((16,)),
        ],
        compiler_params=pltpu.CompilerParams(collective_id=0, has_side_effects=True, vmem_limit_bytes=67043328),
    )(src_times, phi, tau_fwd, tau_bwd, partner.reshape(1, 256))
    return res.reshape(2, 2, 8, 16, 256).transpose(3, 0, 2, 1, 4)


def solution(mesh):
    in_specs = (
        P("op", "tm", None, None, None),
        P(None, "tm", None, None, None),
        P(None, "tm", None, None, None),
        P(),
        P(),
    )
    out_specs = P("op", None, "tm", None, None)
    return jax.shard_map(body, mesh=mesh, in_specs=in_specs, out_specs=out_specs, check_vma=False)
```

```python
import functools

import jax
import jax.numpy as jnp
from jax import lax
from jax.experimental import pallas as pl
from jax.experimental.pallas import tpu as pltpu
from jax.sharding import PartitionSpec as P

MESH = pl.DeviceIdType.MESH
F32 = jnp.float32
BF16 = jnp.bfloat16
NSEM = 208
ROW = 132
COLORS = ((0, 22, "xyz"), (22, 42, "yzx"), (42, 64, "zxy"))
PARTS = (((0, 0, 6), (1, 0, 5)), ((0, 6, 11), (1, 5, 10)), ((0, 11, 16), (1, 10, 16)))
GROUPS = ((0, 0, 4), (3, 0, 4), (1, 0, 4), (2, 0, 2), (2, 2, 2))
XF = 10
ZF = 16 - XF
ZH = ZF // 2


def nxt(v, step):
    return lax.rem(v + step, 4)


def kernel(src, phi, tauf_hbm, taub_hbm, partner, out, S, P2, acc, stage, abuf, fbuf, cand, tauf, taub, fl, wb, rs, comb, dd, rz, rw, ee, rv, comb2,
           send_sem, recv_sem, phi_sem, tau_sem, load_sem):
    op = lax.axis_index("op")
    tm = lax.axis_index("tm")
    core = lax.rem(op, 2)
    zl = op // 8
    zh = lax.rem(tm, 2)
    pos = {"x": tm // 2, "y": lax.rem(op // 2, 4), "z": 2 * zh + zl}

    def device(moved, other_core=False):
        at = dict(pos)
        at.update(moved)
        c = 1 - core if other_core else core
        return ((lax.rem(at["z"], 2) * 4 + at["y"]) * 2 + c, at["x"] * 2 + at["z"] // 2)

    count = [0]
    pending = []

    def send(src_ref, dst_ref, target):
        n = count[0]
        count[0] += 1
        copy = pltpu.make_async_remote_copy(
            src_ref=src_ref, dst_ref=dst_ref, send_sem=send_sem.at[n], recv_sem=recv_sem.at[n],
            device_id=target, device_id_type=MESH)
        copy.start()
        pending.append(copy)
        return copy

    def phi_copy(t):
        slot = lax.rem(t, 2)
        return pltpu.make_async_copy(phi.at[:, t], fbuf.at[slot], phi_sem.at[slot])

    loads = [pltpu.make_async_copy(phi.at[j], P2.at[0, j * 8:j * 8 + 8], load_sem.at[j]) for j in range(16)]
    for copy in loads:
        copy.start()
    peers = [device({d: nxt(pos[d], k)}) for d in "xyz" for k in (1, 3)]
    peers += [device({"z": nxt(pos["z"], 2)}), device({}, True)]
    barrier = pltpu.get_barrier_semaphore()
    for peer in peers:
        pl.semaphore_signal(barrier, inc=1, device_id=peer, device_id_type=MESH)
    taus = [pltpu.make_async_copy(tauf_hbm, tauf, tau_sem.at[0]), pltpu.make_async_copy(taub_hbm, taub, tau_sem.at[1])]
    for copy in taus:
        copy.start()
    phi_copy(0).start()

    for copy in loads:
        copy.wait()
    for s in range(2):
        when = lax.rem(src[s], 8)
        for j in range(16):
            for r in range(2):
                stage[r, j * ROW:j * ROW + 128, :] = P2[0, j * 8 + when, r].astype(F32)

        def deal(ab, c2):
            for q in range(8):
                for r in range(2):
                    rows = stage[r, pl.ds(ab * 8 + q, 16, stride=ROW), :]
                    cand[ab // 4, lax.rem(ab // 2, 2), lax.rem(ab, 2) * 8 + q, s * 2 + r] = rows.astype(BF16)
            return c2

        lax.fori_loop(0, 16, deal, 0)
    acc[...] = jnp.zeros_like(acc)
    for copy in taus:
        copy.wait()
    pl.semaphore_wait(barrier, len(peers))

    def sandwich(t, carry):
        slot = lax.rem(t, 2)
        phi_copy(t).wait()

        @pl.when(t < 7)
        def _():
            phi_copy(t + 1).start()

        for s in range(2):
            fr, fi = tauf[s, t, 0], tauf[s, t, 1]
            fl[0:128, 0:128] = fr
            fl[0:128, 128:256] = -fi
            fl[128:256, 0:128] = fi
            fl[128:256, 128:256] = fr
            br, bi = taub[s, t, 0], taub[s, t, 1]
            wb[0:128, 0:128] = br
            wb[0:128, 128:256] = bi
            wb[128:256, 0:128] = -bi
            wb[128:256, 128:256] = br

            for jp in range(8):
                two = [fbuf[slot, 2 * jp + q].reshape(256, 128) for q in range(2)]
                a = jnp.dot(fl[...], jnp.concatenate(two, axis=1), preferred_element_type=F32).astype(BF16)
                for q in range(2):
                    for r in range(2):
                        abuf[(2 * jp + q) * 128:(2 * jp + q) * 128 + 128, r * 128:r * 128 + 128] = a[r * 128:r * 128 + 128, q * 128:q * 128 + 128]
            for j in range(16):
                prod = jnp.dot(abuf[j * 128:j * 128 + 128, :], wb[...], preferred_element_type=F32)
                for r in range(2):
                    stage[r, j * ROW:j * ROW + 128, :] = prod[:, r * 128:r * 128 + 128]

            def turn(ab, c2):
                for q in range(8):
                    for r in range(2):
                        a = ab * 8 + q
                        rows = stage[r, pl.ds(a, 16, stride=ROW), :]
                        P2[s, a, r, pl.ds(pl.multiple_of(t * 16, 16), 16), :] = rows.astype(BF16)
                return c2

            lax.fori_loop(0, 16, turn, 0)
        return carry

    own_tm = [src[s] // 8 for s in range(2)]
    own_x = [v // 2 for v in own_tm]
    own_zh = [lax.rem(v, 2) for v in own_tm]
    x = pos["x"]
    xp, xm, x2 = nxt(x, 1), nxt(x, 3), nxt(x, 2)
    plus, minus = device({"x": xp}), device({"x": xm})
    far = device({"z": nxt(pos["z"], 2)})

    def choose(s, picks, last):
        value = last
        for condition, other in reversed(picks):
            value = jnp.where(condition[s], other, value)
        return value

    def pick(out_ref, pairs, last):
        for s in range(2):
            h = slice(2 * s, 2 * s + 2)
            out_ref[:, h] = choose(s, [(c, r[:, h]) for c, r in pairs], last[:, h])

    at_x = [v == x for v in own_x]
    at_xp = [v == xp for v in own_x]
    at_xm = [v == xm for v in own_x]
    at_zh = [v == zh for v in own_zh]

    early = pl.ds(0, XF)
    late = pl.ds(XF, ZF)
    pair1 = send(cand.at[:, 1 - zh, late], rz, far)
    first = [
        send(cand.at[x2, 0, early], rs.at[0], plus),
        send(cand.at[x2, 1, early], rs.at[1], minus),
        send(cand.at[xp, 1, early], rs.at[2], plus),
        send(cand.at[xm, 0, early], rs.at[3], minus),
    ]
    lax.fori_loop(0, 2, sandwich, 0)
    first[0].wait_recv()
    first[1].wait_recv()
    pick(comb.at[0], [(at_xm, rs.at[0])], cand.at[xp, 0, early])
    pick(comb.at[1], [(at_xp, rs.at[1])], cand.at[xm, 1, early])
    second = [send(comb.at[0], rs.at[4], plus), send(comb.at[1], rs.at[5], minus)]
    lax.fori_loop(2, 4, sandwich, 0)
    pair1.wait_recv()
    for q in range(4):
        pick(ee.at[q], [(at_zh, cand.at[q, zh, late])], rz.at[q])
    lo, hi = pl.ds(0, ZH), pl.ds(ZH, ZH)
    third = [
        send(ee.at[x2, lo], rv.at[0], plus),
        send(ee.at[x2, hi], rv.at[1], minus),
        send(ee.at[xp, hi], rv.at[2], plus),
        send(ee.at[xm, lo], rv.at[3], minus),
    ]
    for copy in first[2:] + second:
        copy.wait_recv()
    pick(dd.at[0], [(at_x, cand.at[x, 0, early]), (at_xp, rs.at[3])], rs.at[4])
    pick(dd.at[1], [(at_x, cand.at[x, 1, early]), (at_xm, rs.at[2])], rs.at[5])
    pair2 = send(dd.at[1 - zh], rw, far)
    lax.fori_loop(4, 5, sandwich, 0)
    third[0].wait_recv()
    third[1].wait_recv()
    pick(comb2.at[0], [(at_xm, rv.at[0])], ee.at[xp, lo])
    pick(comb2.at[1], [(at_xp, rv.at[1])], ee.at[xm, hi])
    fourth = [send(comb2.at[0], rv.at[4], plus), send(comb2.at[1], rv.at[5], minus)]
    lax.fori_loop(5, 6, sandwich, 0)
    own = S.at[pos["x"], pos["z"], pos["y"], core]
    pair2.wait_recv()
    for a in range(XF):
        for s in range(2):
            h = slice(2 * s, 2 * s + 2)
            own[4 * a + 2 * s:4 * a + 2 * s + 2] = choose(s, [(at_zh, dd[zh, a, h])], rw[a, h])

    whole = pl.ds(0, 4)

    def box(where, lo, hi):
        at = [where[d] for d in "xzy"]
        return S.at[at[0], at[1], at[2], pl.ds(core, 1), pl.ds(lo, hi - lo)]

    def one(v):
        return pl.ds(v, 1)

    mate = device({}, True)
    mate_copies = {(c, k): [] for c in range(3) for k in range(len(GROUPS))}

    def share(color, k, where):
        ref = box(where, *COLORS[color][:2])
        mate_copies[color, k].append(send(ref, ref, mate))

    def ring1(color, d, where):
        lo, hi, _ = COLORS[color]
        w = dict(where)
        w[d] = one(pos[d])
        ref = box(w, lo, hi)
        return [send(ref, ref, device({d: nxt(pos[d], k)})) for k in (1, 3)]

    def ring2(color, d, where):
        lo, hi, _ = COLORS[color]
        mid = (lo + hi) // 2
        w = dict(where)
        w[d] = one(nxt(pos[d], 3))
        a = box(w, lo, mid)
        w[d] = one(nxt(pos[d], 1))
        b = box(w, mid, hi)
        return [send(a, a, device({d: nxt(pos[d], 1)})), send(b, b, device({d: nxt(pos[d], 3)}))]

    def arrived(copies):
        for copy in copies:
            copy.wait_recv()

    three = range(3)
    order = [COLORS[c][2] for c in three]
    base = {d: one(pos[d]) for d in "xyz"}
    p1, p1b, p2, p2b = [None] * 3, [None] * 3, [[] for _ in three], [None] * 3
    p3 = [[[] for _ in GROUPS] for _ in three]
    p3b = [[None] * len(GROUPS) for _ in three]
    line = [dict(base) for _ in three]
    for c in three:
        line[c][order[c][0]] = whole

    def unit(c, u):
        w = dict(base)
        w[order[c][0]] = one(nxt(pos[order[c][0]], u))
        return w

    def second_ring(c, *units):
        for u in units:
            p2[c] += ring1(c, order[c][1], unit(c, u))

    def third_ring(c, *units):
        for u in units:
            p3[c][0] += ring1(c, order[c][2], unit(c, u))

    p1[0] = ring1(0, order[0][0], base)
    second_ring(0, 0)
    third_ring(0, 0)
    for copy in third[2:] + fourth:
        copy.wait_recv()
    for half, mid, side, relay in ((0, at_xp, 3, 4), (1, at_xm, 2, 5)):
        for b in range(ZH):
            a = half * ZH + b
            for s in range(2):
                h = slice(2 * s, 2 * s + 2)
                row = 4 * (XF + a) + 2 * s
                own[row:row + 2] = choose(s, [(at_x, ee[x, a, h]), (mid, rv[side, b, h])], rv[relay, b, h])
    for c in (1, 2):
        p1[c] = ring1(c, order[c][0], base)
    for c in (1, 2):
        second_ring(c, 0)
    for c in (1, 2):
        third_ring(c, 0)
    lax.fori_loop(6, 7, sandwich, 0)
    for c in three:
        arrived(p1[c])
        p1b[c] = ring2(c, order[c][0], base)
    for c in three:
        second_ring(c, 3, 1)
    for c in three:
        arrived(p1b[c])
        second_ring(c, 2)
    for c in three:
        third_ring(c, 3, 1, 2)
        share(c, 0, line[c])

    def group(c, k):
        step, first_place, places = GROUPS[k]
        w = dict(line[c])
        w[order[c][0]] = pl.ds(first_place, places)
        w[order[c][1]] = one(nxt(pos[order[c][1]], step))
        return w

    def spread(c, k):
        p3[c][k] = ring1(c, order[c][2], group(c, k))
        share(c, k, group(c, k))

    lax.fori_loop(7, 8, sandwich, 0)
    for c in three:
        arrived(p2[c])
        p2b[c] = ring2(c, order[c][1], line[c])

    def forward(k):
        for c in three:
            arrived(p3[c][k])
            p3b[c][k] = ring2(c, order[c][2], group(c, k))
            for step in (3, 1):
                w = group(c, k)
                w[order[c][2]] = one(nxt(pos[order[c][2]], step))
                share(c, k, w)

    def settle(k):
        for c in three:
            arrived(p3b[c][k])
            w = group(c, k)
            w[order[c][2]] = one(nxt(pos[order[c][2]], 2))
            share(c, k, w)

    def product(s, p, a0, a1, fields):
        left, right = [], []
        for a in range(a0, a1):
            half = [fields(a * 4 + s * 2 + r) for r in range(2)]
            left.append(jnp.concatenate(half, axis=0))
            right.append(P2[s, p * 16 + a].reshape(256, 128))
        return lax.dot_general(
            jnp.concatenate(left, axis=1), jnp.concatenate(right, axis=1),
            (((1,), (1,)), ((), ())), preferred_element_type=F32)

    def contract(c, k):
        arrived(mate_copies[c, k])
        off, first_place, places = GROUPS[k]
        v = nxt(pos[order[c][1]], off)
        if c == 0:
            def step(p, c2):
                got = [product(*part[:1], p, *part[1:], lambda slab: S[
                    p // 2, pl.ds(lax.rem(p, 2) * 2, 2), v, :, slab].reshape(64, 128)) for part in PARTS[c]]
                for s, value in enumerate(got):
                    acc[s, :, :, v] += value.reshape(2, 2, 32, 256)
                return c2
            lax.fori_loop(2 * first_place, 2 * (first_place + places), step, 0, unroll=2)
        elif c == 1:
            ys = pl.ds(first_place, places)

            def step(xx, c2):
                got = [product(*part[:1], xx * 2 + v // 2, *part[1:], lambda slab: S[
                    xx, v, ys, :, slab].reshape(places * 32, 128)) for part in PARTS[c]]
                for s, value in enumerate(got):
                    acc[s, :, lax.rem(v, 2), ys] += value.reshape(2, places, 32, 256)
                return c2
            lax.fori_loop(0, 4, step, 0, unroll=2)
        else:
            for h in range(first_place // 2, (first_place + places) // 2):
                for part in PARTS[c]:
                    got = product(*part[:1], v * 2 + h, *part[1:], lambda slab: S[
                        v, 2 * h:2 * h + 2, :, :, slab].reshape(256, 128))
                    acc[part[0]] += got.reshape(2, 2, 4, 32, 256)

    def contract_all(k):
        for c in three:
            contract(c, k)

    def spread_all(k):
        for c in three:
            spread(c, k)

    forward(0)
    spread_all(1)
    spread_all(2)
    for c in three:
        arrived(p2b[c])
    settle(0)
    contract_all(0)
    forward(1)
    spread_all(3)
    forward(2)
    spread_all(4)
    settle(1)
    contract_all(1)
    forward(3)
    settle(2)
    forward(4)
    contract_all(2)
    settle(3)
    contract_all(3)
    settle(4)
    contract_all(4)

    hot = (partner[...] == lax.broadcasted_iota(jnp.int32, (256, 256), 0)).astype(F32)
    for s in range(2):
        q = acc[s].reshape(512, 256)
        real = q[0:256, 0:128] + q[256:512, 128:256]
        imag = q[0:256, 128:256] - q[256:512, 0:128]
        for r, v in enumerate((real, imag)):
            got = lax.dot_general(v, hot, (((0,), (0,)), ((), ())), precision=lax.Precision.HIGHEST,
                                  preferred_element_type=F32)
            out[s, r] = got * (1.0 / 128.0)
    for copy in pending:
        copy.wait_send()


def body(phi, tau_fwd, tau_bwd, src_times, partner):
    vm = pl.BlockSpec(memory_space=pltpu.VMEM)
    hbm = pl.BlockSpec(memory_space=pl.ANY)
    res = pl.pallas_call(
        kernel,
        out_shape=jax.ShapeDtypeStruct((2, 2, 128, 256), F32),
        in_specs=[pl.BlockSpec(memory_space=pltpu.SMEM), hbm, hbm, hbm, vm],
        out_specs=vm,
        scratch_shapes=[
            pltpu.VMEM((4, 4, 4, 2, 64, 16, 128), BF16),
            pltpu.VMEM((2, 128, 2, 128, 128), BF16),
            pltpu.VMEM((2, 2, 2, 4, 32, 256), F32),
            pltpu.VMEM((2, 16 * ROW, 128), F32),
            pltpu.VMEM((2048, 256), BF16),
            pltpu.VMEM((2, 16, 2, 128, 128), BF16),
            pltpu.VMEM((4, 2, 16, 4, 16, 128), BF16),
            pltpu.VMEM((2, 8, 2, 128, 128), BF16),
            pltpu.VMEM((2, 8, 2, 128, 128), BF16),
            pltpu.VMEM((256, 256), BF16),
            pltpu.VMEM((256, 256), BF16),
            pltpu.VMEM((6, XF, 4, 16, 128), BF16),
            pltpu.VMEM((2, XF, 4, 16, 128), BF16),
            pltpu.VMEM((2, XF, 4, 16, 128), BF16),
            pltpu.VMEM((4, ZF, 4, 16, 128), BF16),
            pltpu.VMEM((XF, 4, 16, 128), BF16),
            pltpu.VMEM((4, ZF, 4, 16, 128), BF16),
            pltpu.VMEM((6, ZH, 4, 16, 128), BF16),
            pltpu.VMEM((2, ZH, 4, 16, 128), BF16),
            pltpu.SemaphoreType.DMA((NSEM,)),
            pltpu.SemaphoreType.DMA((NSEM,)),
            pltpu.SemaphoreType.DMA((2,)),
            pltpu.SemaphoreType.DMA((2,)),
            pltpu.SemaphoreType.DMA((16,)),
        ],
        compiler_params=pltpu.CompilerParams(collective_id=0, has_side_effects=True, vmem_limit_bytes=67043328),
    )(src_times, phi, tau_fwd, tau_bwd, partner.reshape(1, 256))
    return res.reshape(2, 2, 8, 16, 256).transpose(3, 0, 2, 1, 4)


def solution(mesh):
    in_specs = (
        P("op", "tm", None, None, None),
        P(None, "tm", None, None, None),
        P(None, "tm", None, None, None),
        P(),
        P(),
    )
    out_specs = P("op", None, "tm", None, None)
    return jax.shard_map(body, mesh=mesh, in_specs=in_specs, out_specs=out_specs, check_vma=False)
```

```python
import functools

import jax
import jax.numpy as jnp
from jax import lax
from jax.experimental import pallas as pl
from jax.experimental.pallas import tpu as pltpu
from jax.sharding import PartitionSpec as P

MESH = pl.DeviceIdType.MESH
F32 = jnp.float32
BF16 = jnp.bfloat16
NSEM = 208
ROW = 132
COLORS = ((0, 22, "xyz"), (22, 42, "yzx"), (42, 64, "zxy"))
PARTS = (((0, 0, 6), (1, 0, 5)), ((0, 6, 11), (1, 5, 10)), ((0, 11, 16), (1, 10, 16)))
GROUPS = ((0, 0, 4), (3, 0, 4), (1, 0, 4), (2, 0, 2), (2, 2, 2))
XF = 10
ZF = 16 - XF
ZH = ZF // 2


def nxt(v, step):
    return lax.rem(v + step, 4)


def kernel(src, phi, tauf_hbm, taub_hbm, partner, out, S, P2, acc, stage, abuf, fbuf, cand, tauf, taub, fl, wb, rs, comb, dd, rz, rw, ee, rv, comb2,
           send_sem, recv_sem, phi_sem, tau_sem, load_sem):
    op = lax.axis_index("op")
    tm = lax.axis_index("tm")
    core = lax.rem(op, 2)
    zl = op // 8
    zh = lax.rem(tm, 2)
    pos = {"x": tm // 2, "y": lax.rem(op // 2, 4), "z": 2 * zh + zl}

    def device(moved, other_core=False):
        at = dict(pos)
        at.update(moved)
        c = 1 - core if other_core else core
        return ((lax.rem(at["z"], 2) * 4 + at["y"]) * 2 + c, at["x"] * 2 + at["z"] // 2)

    count = [0]
    pending = []

    def send(src_ref, dst_ref, target):
        n = count[0]
        count[0] += 1
        copy = pltpu.make_async_remote_copy(
            src_ref=src_ref, dst_ref=dst_ref, send_sem=send_sem.at[n], recv_sem=recv_sem.at[n],
            device_id=target, device_id_type=MESH)
        copy.start()
        pending.append(copy)
        return copy

    def phi_copy(t):
        slot = lax.rem(t, 2)
        return pltpu.make_async_copy(phi.at[:, t], fbuf.at[slot], phi_sem.at[slot])

    loads = [pltpu.make_async_copy(phi.at[j], P2.at[0, j * 8:j * 8 + 8], load_sem.at[j]) for j in range(16)]
    for copy in loads:
        copy.start()
    peers = [device({d: nxt(pos[d], k)}) for d in "xyz" for k in (1, 3)]
    peers += [device({"z": nxt(pos["z"], 2)}), device({}, True)]
    barrier = pltpu.get_barrier_semaphore()
    for peer in peers:
        pl.semaphore_signal(barrier, inc=1, device_id=peer, device_id_type=MESH)
    taus = [pltpu.make_async_copy(tauf_hbm, tauf, tau_sem.at[0]), pltpu.make_async_copy(taub_hbm, taub, tau_sem.at[1])]
    for copy in taus:
        copy.start()
    phi_copy(0).start()

    for copy in loads:
        copy.wait()
    for s in range(2):
        when = lax.rem(src[s], 8)
        for j in range(16):
            for r in range(2):
                stage[r, j * ROW:j * ROW + 128, :] = P2[0, j * 8 + when, r].astype(F32)

        def deal(ab, c2):
            for q in range(8):
                for r in range(2):
                    rows = stage[r, pl.ds(ab * 8 + q, 16, stride=ROW), :]
                    cand[ab // 4, lax.rem(ab // 2, 2), lax.rem(ab, 2) * 8 + q, s * 2 + r] = rows.astype(BF16)
            return c2

        lax.fori_loop(0, 16, deal, 0)
    acc[...] = jnp.zeros_like(acc)
    for copy in taus:
        copy.wait()
    pl.semaphore_wait(barrier, len(peers))

    def sandwich(t, carry):
        slot = lax.rem(t, 2)
        phi_copy(t).wait()

        @pl.when(t < 7)
        def _():
            phi_copy(t + 1).start()

        for s in range(2):
            fr, fi = tauf[s, t, 0], tauf[s, t, 1]
            fl[0:128, 0:128] = fr
            fl[0:128, 128:256] = -fi
            fl[128:256, 0:128] = fi
            fl[128:256, 128:256] = fr
            br, bi = taub[s, t, 0], taub[s, t, 1]
            wb[0:128, 0:128] = br
            wb[0:128, 128:256] = bi
            wb[128:256, 0:128] = -bi
            wb[128:256, 128:256] = br

            for jp in range(8):
                two = [fbuf[slot, 2 * jp + q].reshape(256, 128) for q in range(2)]
                a = jnp.dot(fl[...], jnp.concatenate(two, axis=1), preferred_element_type=F32).astype(BF16)
                for q in range(2):
                    for r in range(2):
                        abuf[(2 * jp + q) * 128:(2 * jp + q) * 128 + 128, r * 128:r * 128 + 128] = a[r * 128:r * 128 + 128, q * 128:q * 128 + 128]
            for j in range(16):
                prod = jnp.dot(abuf[j * 128:j * 128 + 128, :], wb[...], preferred_element_type=F32)
                for r in range(2):
                    stage[r, j * ROW:j * ROW + 128, :] = prod[:, r * 128:r * 128 + 128]

            def turn(ab, c2):
                for q in range(8):
                    for r in range(2):
                        a = ab * 8 + q
                        rows = stage[r, pl.ds(a, 16, stride=ROW), :]
                        P2[s, a, r, pl.ds(pl.multiple_of(t * 16, 16), 16), :] = rows.astype(BF16)
                return c2

            lax.fori_loop(0, 16, turn, 0)
        return carry

    own_tm = [src[s] // 8 for s in range(2)]
    own_x = [v // 2 for v in own_tm]
    own_zh = [lax.rem(v, 2) for v in own_tm]
    x = pos["x"]
    xp, xm, x2 = nxt(x, 1), nxt(x, 3), nxt(x, 2)
    plus, minus = device({"x": xp}), device({"x": xm})
    far = device({"z": nxt(pos["z"], 2)})

    def choose(s, picks, last):
        value = last
        for condition, other in reversed(picks):
            value = jnp.where(condition[s], other, value)
        return value

    def pick(out_ref, pairs, last):
        for s in range(2):
            h = slice(2 * s, 2 * s + 2)
            out_ref[:, h] = choose(s, [(c, r[:, h]) for c, r in pairs], last[:, h])

    at_x = [v == x for v in own_x]
    at_xp = [v == xp for v in own_x]
    at_xm = [v == xm for v in own_x]
    at_zh = [v == zh for v in own_zh]

    early = pl.ds(0, XF)
    late = pl.ds(XF, ZF)
    pair1 = send(cand.at[:, 1 - zh, late], rz, far)
    first = [
        send(cand.at[x2, 0, early], rs.at[0], plus),
        send(cand.at[x2, 1, early], rs.at[1], minus),
        send(cand.at[xp, 1, early], rs.at[2], plus),
        send(cand.at[xm, 0, early], rs.at[3], minus),
    ]
    lax.fori_loop(0, 2, sandwich, 0)
    first[0].wait_recv()
    first[1].wait_recv()
    pick(comb.at[0], [(at_xm, rs.at[0])], cand.at[xp, 0, early])
    pick(comb.at[1], [(at_xp, rs.at[1])], cand.at[xm, 1, early])
    second = [send(comb.at[0], rs.at[4], plus), send(comb.at[1], rs.at[5], minus)]
    lax.fori_loop(2, 4, sandwich, 0)
    pair1.wait_recv()
    for q in range(4):
        pick(ee.at[q], [(at_zh, cand.at[q, zh, late])], rz.at[q])
    lo, hi = pl.ds(0, ZH), pl.ds(ZH, ZH)
    third = [
        send(ee.at[x2, lo], rv.at[0], plus),
        send(ee.at[x2, hi], rv.at[1], minus),
        send(ee.at[xp, hi], rv.at[2], plus),
        send(ee.at[xm, lo], rv.at[3], minus),
    ]
    for copy in first[2:] + second:
        copy.wait_recv()
    pick(dd.at[0], [(at_x, cand.at[x, 0, early]), (at_xp, rs.at[3])], rs.at[4])
    pick(dd.at[1], [(at_x, cand.at[x, 1, early]), (at_xm, rs.at[2])], rs.at[5])
    pair2 = send(dd.at[1 - zh], rw, far)
    lax.fori_loop(4, 5, sandwich, 0)
    third[0].wait_recv()
    third[1].wait_recv()
    pick(comb2.at[0], [(at_xm, rv.at[0])], ee.at[xp, lo])
    pick(comb2.at[1], [(at_xp, rv.at[1])], ee.at[xm, hi])
    fourth = [send(comb2.at[0], rv.at[4], plus), send(comb2.at[1], rv.at[5], minus)]
    lax.fori_loop(5, 6, sandwich, 0)
    own = S.at[pos["x"], pos["z"], pos["y"], core]
    pair2.wait_recv()
    for a in range(XF):
        for s in range(2):
            h = slice(2 * s, 2 * s + 2)
            own[4 * a + 2 * s:4 * a + 2 * s + 2] = choose(s, [(at_zh, dd[zh, a, h])], rw[a, h])

    whole = pl.ds(0, 4)

    def box(where, lo, hi):
        at = [where[d] for d in "xzy"]
        return S.at[at[0], at[1], at[2], pl.ds(core, 1), pl.ds(lo, hi - lo)]

    def one(v):
        return pl.ds(v, 1)

    mate = device({}, True)
    mate_copies = {(c, k): [] for c in range(3) for k in range(len(GROUPS))}

    def share(color, k, where):
        ref = box(where, *COLORS[color][:2])
        mate_copies[color, k].append(send(ref, ref, mate))

    def ring1(color, d, where):
        lo, hi, _ = COLORS[color]
        w = dict(where)
        w[d] = one(pos[d])
        ref = box(w, lo, hi)
        return [send(ref, ref, device({d: nxt(pos[d], k)})) for k in (1, 3)]

    def ring2(color, d, where):
        lo, hi, _ = COLORS[color]
        mid = (lo + hi) // 2
        w = dict(where)
        w[d] = one(nxt(pos[d], 3))
        a = box(w, lo, mid)
        w[d] = one(nxt(pos[d], 1))
        b = box(w, mid, hi)
        return [send(a, a, device({d: nxt(pos[d], 1)})), send(b, b, device({d: nxt(pos[d], 3)}))]

    def arrived(copies):
        for copy in copies:
            copy.wait_recv()

    three = range(3)
    order = [COLORS[c][2] for c in three]
    base = {d: one(pos[d]) for d in "xyz"}
    p1, p1b, p2, p2b = [None] * 3, [None] * 3, [[] for _ in three], [None] * 3
    p3 = [[[] for _ in GROUPS] for _ in three]
    p3b = [[None] * len(GROUPS) for _ in three]
    line = [dict(base) for _ in three]
    for c in three:
        line[c][order[c][0]] = whole

    def unit(c, u):
        w = dict(base)
        w[order[c][0]] = one(nxt(pos[order[c][0]], u))
        return w

    def second_ring(c, *units):
        for u in units:
            p2[c] += ring1(c, order[c][1], unit(c, u))

    def third_ring(c, *units):
        for u in units:
            p3[c][0] += ring1(c, order[c][2], unit(c, u))

    p1[0] = ring1(0, order[0][0], base)
    second_ring(0, 0)
    third_ring(0, 0)
    for copy in third[2:] + fourth:
        copy.wait_recv()
    for half, mid, side, relay in ((0, at_xp, 3, 4), (1, at_xm, 2, 5)):
        for b in range(ZH):
            a = half * ZH + b
            for s in range(2):
                h = slice(2 * s, 2 * s + 2)
                row = 4 * (XF + a) + 2 * s
                own[row:row + 2] = choose(s, [(at_x, ee[x, a, h]), (mid, rv[side, b, h])], rv[relay, b, h])
    for c in (1, 2):
        p1[c] = ring1(c, order[c][0], base)
    for c in (1, 2):
        second_ring(c, 0)
    for c in (1, 2):
        third_ring(c, 0)
    lax.fori_loop(6, 7, sandwich, 0)
    for c in three:
        arrived(p1[c])
        p1b[c] = ring2(c, order[c][0], base)
    for c in three:
        second_ring(c, 3, 1)
    for c in three:
        arrived(p1b[c])
        second_ring(c, 2)
    for c in three:
        third_ring(c, 3, 1, 2)
        share(c, 0, line[c])

    def group(c, k):
        step, first_place, places = GROUPS[k]
        w = dict(line[c])
        w[order[c][0]] = pl.ds(first_place, places)
        w[order[c][1]] = one(nxt(pos[order[c][1]], step))
        return w

    def spread(c, k):
        p3[c][k] = ring1(c, order[c][2], group(c, k))
        share(c, k, group(c, k))

    lax.fori_loop(7, 8, sandwich, 0)
    for c in three:
        arrived(p2[c])
        p2b[c] = ring2(c, order[c][1], line[c])

    def forward(k):
        for c in three:
            arrived(p3[c][k])
            p3b[c][k] = ring2(c, order[c][2], group(c, k))
            for step in (3, 1):
                w = group(c, k)
                w[order[c][2]] = one(nxt(pos[order[c][2]], step))
                share(c, k, w)

    def settle(k):
        for c in three:
            arrived(p3b[c][k])
            w = group(c, k)
            w[order[c][2]] = one(nxt(pos[order[c][2]], 2))
            share(c, k, w)

    def product(s, p, a0, a1, fields):
        left, right = [], []
        for a in range(a0, a1):
            half = [fields(a * 4 + s * 2 + r) for r in range(2)]
            left.append(jnp.concatenate(half, axis=0))
            right.append(P2[s, p * 16 + a].reshape(256, 128))
        return lax.dot_general(
            jnp.concatenate(left, axis=1), jnp.concatenate(right, axis=1),
            (((1,), (1,)), ((), ())), preferred_element_type=F32)

    def contract(c, k, base_off, n_off, copies):
        arrived(copies)
        off, first_place, places = GROUPS[k]
        v = nxt(pos[order[c][1]], off)
        if c == 0:
            def step(i, c2):
                z = nxt(pos["z"], base_off + i // places)
                xx = first_place + lax.rem(i, places)
                got = [product(*part[:1], xx * 2 + z // 2, *part[1:], lambda slab: S[
                    xx, z, v, :, slab].reshape(32, 128)) for part in PARTS[c]]
                for s, value in enumerate(got):
                    acc[s, :, lax.rem(z, 2), v] += value.reshape(2, 32, 256)
                return c2
            lax.fori_loop(0, n_off * places, step, 0, unroll=2)
        elif c == 1:
            ys = pl.ds(first_place, places)
            for i in range(n_off):
                xx = nxt(pos["x"], base_off + i)
                got = [product(*part[:1], xx * 2 + v // 2, *part[1:], lambda slab: S[
                    xx, v, ys, :, slab].reshape(places * 32, 128)) for part in PARTS[c]]
                for s, value in enumerate(got):
                    acc[s, :, lax.rem(v, 2), ys] += value.reshape(2, places, 32, 256)
        else:
            for i in range(n_off):
                y = nxt(pos["y"], base_off + i)
                for half in range(first_place // 2, (first_place + places) // 2):
                    got = [product(*part[:1], v * 2 + half, *part[1:], lambda slab: S[
                        v, 2 * half:2 * half + 2, y, :, slab].reshape(64, 128)) for part in PARTS[c]]
                    for s, value in enumerate(got):
                        acc[s, :, :, y] += value.reshape(2, 2, 32, 256)

    def early(k):
        for c in three:
            contract(c, k, 3, 3, mate_copies[c, k][:3])

    def late(k):
        for c in three:
            contract(c, k, 2, 1, mate_copies[c, k][3:])

    def spread_all(k):
        for c in three:
            spread(c, k)

    forward(0)
    spread_all(1)
    spread_all(2)
    for c in three:
        arrived(p2b[c])
    early(0)
    settle(0)
    late(0)
    forward(1)
    spread_all(3)
    early(1)
    forward(2)
    spread_all(4)
    settle(1)
    early(2)
    forward(3)
    late(1)
    settle(2)
    early(3)
    late(2)
    forward(4)
    settle(3)
    early(4)
    settle(4)
    late(3)
    late(4)

    hot = (partner[...] == lax.broadcasted_iota(jnp.int32, (256, 256), 0)).astype(F32)
    for s in range(2):
        q = acc[s].reshape(512, 256)
        real = q[0:256, 0:128] + q[256:512, 128:256]
        imag = q[0:256, 128:256] - q[256:512, 0:128]
        for r, v in enumerate((real, imag)):
            got = lax.dot_general(v, hot, (((0,), (0,)), ((), ())), precision=lax.Precision.HIGHEST,
                                  preferred_element_type=F32)
            out[s, r] = got * (1.0 / 128.0)
    for copy in pending:
        copy.wait_send()


def body(phi, tau_fwd, tau_bwd, src_times, partner):
    vm = pl.BlockSpec(memory_space=pltpu.VMEM)
    hbm = pl.BlockSpec(memory_space=pl.ANY)
    res = pl.pallas_call(
        kernel,
        out_shape=jax.ShapeDtypeStruct((2, 2, 128, 256), F32),
        in_specs=[pl.BlockSpec(memory_space=pltpu.SMEM), hbm, hbm, hbm, vm],
        out_specs=vm,
        scratch_shapes=[
            pltpu.VMEM((4, 4, 4, 2, 64, 16, 128), BF16),
            pltpu.VMEM((2, 128, 2, 128, 128), BF16),
            pltpu.VMEM((2, 2, 2, 4, 32, 256), F32),
            pltpu.VMEM((2, 16 * ROW, 128), F32),
            pltpu.VMEM((2048, 256), BF16),
            pltpu.VMEM((2, 16, 2, 128, 128), BF16),
            pltpu.VMEM((4, 2, 16, 4, 16, 128), BF16),
            pltpu.VMEM((2, 8, 2, 128, 128), BF16),
            pltpu.VMEM((2, 8, 2, 128, 128), BF16),
            pltpu.VMEM((256, 256), BF16),
            pltpu.VMEM((256, 256), BF16),
            pltpu.VMEM((6, XF, 4, 16, 128), BF16),
            pltpu.VMEM((2, XF, 4, 16, 128), BF16),
            pltpu.VMEM((2, XF, 4, 16, 128), BF16),
            pltpu.VMEM((4, ZF, 4, 16, 128), BF16),
            pltpu.VMEM((XF, 4, 16, 128), BF16),
            pltpu.VMEM((4, ZF, 4, 16, 128), BF16),
            pltpu.VMEM((6, ZH, 4, 16, 128), BF16),
            pltpu.VMEM((2, ZH, 4, 16, 128), BF16),
            pltpu.SemaphoreType.DMA((NSEM,)),
            pltpu.SemaphoreType.DMA((NSEM,)),
            pltpu.SemaphoreType.DMA((2,)),
            pltpu.SemaphoreType.DMA((2,)),
            pltpu.SemaphoreType.DMA((16,)),
        ],
        compiler_params=pltpu.CompilerParams(collective_id=0, has_side_effects=True, vmem_limit_bytes=67043328),
    )(src_times, phi, tau_fwd, tau_bwd, partner.reshape(1, 256))
    return res.reshape(2, 2, 8, 16, 256).transpose(3, 0, 2, 1, 4)


def solution(mesh):
    in_specs = (
        P("op", "tm", None, None, None),
        P(None, "tm", None, None, None),
        P(None, "tm", None, None, None),
        P(),
        P(),
    )
    out_specs = P("op", None, "tm", None, None)
    return jax.shard_map(body, mesh=mesh, in_specs=in_specs, out_specs=out_specs, check_vma=False)
```

```python
import functools

import jax
import jax.numpy as jnp
from jax import lax
from jax.experimental import pallas as pl
from jax.experimental.pallas import tpu as pltpu
from jax.sharding import PartitionSpec as P

MESH = pl.DeviceIdType.MESH
F32 = jnp.float32
BF16 = jnp.bfloat16
NSEM = 208
ROW = 132
COLORS = ((0, 22, "xyz"), (22, 42, "yzx"), (42, 64, "zxy"))
PARTS = (((0, 0, 6), (1, 0, 5)), ((0, 6, 11), (1, 5, 10)), ((0, 11, 16), (1, 10, 16)))
GROUPS = ((0, 0, 4), (3, 0, 4), (1, 0, 4), (2, 0, 2), (2, 2, 2))
XF = 10
ZF = 16 - XF
ZH = ZF // 2


def nxt(v, step):
    return lax.rem(v + step, 4)


def kernel(src, phi, tauf_hbm, taub_hbm, partner, out, S, P2, acc, stage, abuf, fbuf, cand, tauf, taub, fl, wb, rs, comb, dd, rz, rw, ee, rv, comb2,
           send_sem, recv_sem, phi_sem, tau_sem, load_sem):
    op = lax.axis_index("op")
    tm = lax.axis_index("tm")
    core = lax.rem(op, 2)
    zl = op // 8
    zh = lax.rem(tm, 2)
    pos = {"x": tm // 2, "y": lax.rem(op // 2, 4), "z": 2 * zh + zl}

    def device(moved, other_core=False):
        at = dict(pos)
        at.update(moved)
        c = 1 - core if other_core else core
        return ((lax.rem(at["z"], 2) * 4 + at["y"]) * 2 + c, at["x"] * 2 + at["z"] // 2)

    count = [0]
    pending = []

    def send(src_ref, dst_ref, target):
        n = count[0]
        count[0] += 1
        copy = pltpu.make_async_remote_copy(
            src_ref=src_ref, dst_ref=dst_ref, send_sem=send_sem.at[n], recv_sem=recv_sem.at[n],
            device_id=target, device_id_type=MESH)
        copy.start()
        pending.append(copy)
        return copy

    def phi_copy(t):
        slot = lax.rem(t, 2)
        return pltpu.make_async_copy(phi.at[:, t], fbuf.at[slot], phi_sem.at[slot])

    loads = [pltpu.make_async_copy(phi.at[j], P2.at[0, j * 8:j * 8 + 8], load_sem.at[j]) for j in range(16)]
    for copy in loads:
        copy.start()
    peers = [device({d: nxt(pos[d], k)}) for d in "xyz" for k in (1, 3)]
    peers += [device({"z": nxt(pos["z"], 2)}), device({}, True)]
    barrier = pltpu.get_barrier_semaphore()
    for peer in peers:
        pl.semaphore_signal(barrier, inc=1, device_id=peer, device_id_type=MESH)
    taus = [pltpu.make_async_copy(tauf_hbm, tauf, tau_sem.at[0]), pltpu.make_async_copy(taub_hbm, taub, tau_sem.at[1])]

    for copy in loads:
        copy.wait()
    for copy in taus:
        copy.start()
    phi_copy(0).start()
    for s in range(2):
        when = lax.rem(src[s], 8)
        for j in range(16):
            for r in range(2):
                stage[r, j * ROW:j * ROW + 128, :] = P2[0, j * 8 + when, r].astype(F32)

        def deal(ab, c2):
            for q in range(8):
                for r in range(2):
                    rows = stage[r, pl.ds(ab * 8 + q, 16, stride=ROW), :]
                    cand[ab // 4, lax.rem(ab // 2, 2), lax.rem(ab, 2) * 8 + q, s * 2 + r] = rows.astype(BF16)
            return c2

        lax.fori_loop(0, 16, deal, 0, unroll=4)
    pl.semaphore_wait(barrier, len(peers))

    def sandwich(t, carry):
        slot = lax.rem(t, 2)
        phi_copy(t).wait()

        @pl.when(t < 7)
        def _():
            phi_copy(t + 1).start()

        for s in range(2):
            fr, fi = tauf[s, t, 0], tauf[s, t, 1]
            fl[0:128, 0:128] = fr
            fl[0:128, 128:256] = -fi
            fl[128:256, 0:128] = fi
            fl[128:256, 128:256] = fr
            br, bi = taub[s, t, 0], taub[s, t, 1]
            wb[0:128, 0:128] = br
            wb[0:128, 128:256] = bi
            wb[128:256, 0:128] = -bi
            wb[128:256, 128:256] = br

            for jp in range(8):
                two = [fbuf[slot, 2 * jp + q].reshape(256, 128) for q in range(2)]
                a = jnp.dot(fl[...], jnp.concatenate(two, axis=1), preferred_element_type=F32).astype(BF16)
                for q in range(2):
                    for r in range(2):
                        abuf[(2 * jp + q) * 128:(2 * jp + q) * 128 + 128, r * 128:r * 128 + 128] = a[r * 128:r * 128 + 128, q * 128:q * 128 + 128]
            for j in range(16):
                prod = jnp.dot(abuf[j * 128:j * 128 + 128, :], wb[...], preferred_element_type=F32)
                for r in range(2):
                    stage[r, j * ROW:j * ROW + 128, :] = prod[:, r * 128:r * 128 + 128]

            def turn(ab, c2):
                for q in range(8):
                    for r in range(2):
                        a = ab * 8 + q
                        rows = stage[r, pl.ds(a, 16, stride=ROW), :]
                        P2[s, a, r, pl.ds(pl.multiple_of(t * 16, 16), 16), :] = rows.astype(BF16)
                return c2

            lax.fori_loop(0, 16, turn, 0)
        return carry

    own_tm = [src[s] // 8 for s in range(2)]
    own_x = [v // 2 for v in own_tm]
    own_zh = [lax.rem(v, 2) for v in own_tm]
    x = pos["x"]
    xp, xm, x2 = nxt(x, 1), nxt(x, 3), nxt(x, 2)
    plus, minus = device({"x": xp}), device({"x": xm})
    far = device({"z": nxt(pos["z"], 2)})

    def choose(s, picks, last):
        value = last
        for condition, other in reversed(picks):
            value = jnp.where(condition[s], other, value)
        return value

    def pick(out_ref, pairs, last):
        for s in range(2):
            h = slice(2 * s, 2 * s + 2)
            out_ref[:, h] = choose(s, [(c, r[:, h]) for c, r in pairs], last[:, h])

    at_x = [v == x for v in own_x]
    at_xp = [v == xp for v in own_x]
    at_xm = [v == xm for v in own_x]
    at_zh = [v == zh for v in own_zh]

    early = pl.ds(0, XF)
    late = pl.ds(XF, ZF)
    pair1 = send(cand.at[:, 1 - zh, late], rz, far)
    first = [
        send(cand.at[x2, 0, early], rs.at[0], plus),
        send(cand.at[x2, 1, early], rs.at[1], minus),
        send(cand.at[xp, 1, early], rs.at[2], plus),
        send(cand.at[xm, 0, early], rs.at[3], minus),
    ]
    acc[...] = jnp.zeros_like(acc)
    for copy in taus:
        copy.wait()
    lax.fori_loop(0, 2, sandwich, 0)
    first[0].wait_recv()
    first[1].wait_recv()
    pick(comb.at[0], [(at_xm, rs.at[0])], cand.at[xp, 0, early])
    pick(comb.at[1], [(at_xp, rs.at[1])], cand.at[xm, 1, early])
    second = [send(comb.at[0], rs.at[4], plus), send(comb.at[1], rs.at[5], minus)]
    lax.fori_loop(2, 4, sandwich, 0)
    pair1.wait_recv()
    for q in range(4):
        pick(ee.at[q], [(at_zh, cand.at[q, zh, late])], rz.at[q])
    lo, hi = pl.ds(0, ZH), pl.ds(ZH, ZH)
    third = [
        send(ee.at[x2, lo], rv.at[0], plus),
        send(ee.at[x2, hi], rv.at[1], minus),
        send(ee.at[xp, hi], rv.at[2], plus),
        send(ee.at[xm, lo], rv.at[3], minus),
    ]
    for copy in first[2:] + second:
        copy.wait_recv()
    pick(dd.at[0], [(at_x, cand.at[x, 0, early]), (at_xp, rs.at[3])], rs.at[4])
    pick(dd.at[1], [(at_x, cand.at[x, 1, early]), (at_xm, rs.at[2])], rs.at[5])
    pair2 = send(dd.at[1 - zh], rw, far)
    lax.fori_loop(4, 5, sandwich, 0)
    third[0].wait_recv()
    third[1].wait_recv()
    pick(comb2.at[0], [(at_xm, rv.at[0])], ee.at[xp, lo])
    pick(comb2.at[1], [(at_xp, rv.at[1])], ee.at[xm, hi])
    fourth = [send(comb2.at[0], rv.at[4], plus), send(comb2.at[1], rv.at[5], minus)]
    lax.fori_loop(5, 6, sandwich, 0)
    own = S.at[pos["x"], pos["z"], pos["y"], core]
    pair2.wait_recv()
    for a in range(XF):
        for s in range(2):
            h = slice(2 * s, 2 * s + 2)
            own[4 * a + 2 * s:4 * a + 2 * s + 2] = choose(s, [(at_zh, dd[zh, a, h])], rw[a, h])

    whole = pl.ds(0, 4)

    def box(where, lo, hi):
        at = [where[d] for d in "xzy"]
        return S.at[at[0], at[1], at[2], pl.ds(core, 1), pl.ds(lo, hi - lo)]

    def one(v):
        return pl.ds(v, 1)

    mate = device({}, True)
    mate_copies = {(c, k): [] for c in range(3) for k in range(len(GROUPS))}

    def share(color, k, where):
        ref = box(where, *COLORS[color][:2])
        mate_copies[color, k].append(send(ref, ref, mate))

    def ring1(color, d, where):
        lo, hi, _ = COLORS[color]
        w = dict(where)
        w[d] = one(pos[d])
        ref = box(w, lo, hi)
        return [send(ref, ref, device({d: nxt(pos[d], k)})) for k in (1, 3)]

    def ring2(color, d, where):
        lo, hi, _ = COLORS[color]
        mid = (lo + hi) // 2
        w = dict(where)
        w[d] = one(nxt(pos[d], 3))
        a = box(w, lo, mid)
        w[d] = one(nxt(pos[d], 1))
        b = box(w, mid, hi)
        return [send(a, a, device({d: nxt(pos[d], 1)})), send(b, b, device({d: nxt(pos[d], 3)}))]

    def arrived(copies):
        for copy in copies:
            copy.wait_recv()

    three = range(3)
    order = [COLORS[c][2] for c in three]
    base = {d: one(pos[d]) for d in "xyz"}
    p1, p1b, p2, p2b = [None] * 3, [None] * 3, [[] for _ in three], [None] * 3
    p3 = [[[] for _ in GROUPS] for _ in three]
    p3b = [[None] * len(GROUPS) for _ in three]
    line = [dict(base) for _ in three]
    for c in three:
        line[c][order[c][0]] = whole

    def unit(c, u):
        w = dict(base)
        w[order[c][0]] = one(nxt(pos[order[c][0]], u))
        return w

    def second_ring(c, *units):
        for u in units:
            p2[c] += ring1(c, order[c][1], unit(c, u))

    def third_ring(c, *units):
        for u in units:
            p3[c][0] += ring1(c, order[c][2], unit(c, u))

    p1[0] = ring1(0, order[0][0], base)
    second_ring(0, 0)
    third_ring(0, 0)
    for copy in third[2:] + fourth:
        copy.wait_recv()
    for half, mid, side, relay in ((0, at_xp, 3, 4), (1, at_xm, 2, 5)):
        for b in range(ZH):
            a = half * ZH + b
            for s in range(2):
                h = slice(2 * s, 2 * s + 2)
                row = 4 * (XF + a) + 2 * s
                own[row:row + 2] = choose(s, [(at_x, ee[x, a, h]), (mid, rv[side, b, h])], rv[relay, b, h])
    for c in (1, 2):
        p1[c] = ring1(c, order[c][0], base)
    for c in (1, 2):
        second_ring(c, 0)
    for c in (1, 2):
        third_ring(c, 0)
    lax.fori_loop(6, 7, sandwich, 0)
    for c in three:
        arrived(p1[c])
        p1b[c] = ring2(c, order[c][0], base)
    for c in three:
        second_ring(c, 3, 1)
    for c in three:
        arrived(p1b[c])
        second_ring(c, 2)
    for c in three:
        third_ring(c, 3, 1, 2)
        share(c, 0, line[c])

    def group(c, k):
        step, first_place, places = GROUPS[k]
        w = dict(line[c])
        w[order[c][0]] = pl.ds(first_place, places)
        w[order[c][1]] = one(nxt(pos[order[c][1]], step))
        return w

    def spread(c, k):
        p3[c][k] = ring1(c, order[c][2], group(c, k))
        share(c, k, group(c, k))

    lax.fori_loop(7, 8, sandwich, 0)
    for c in three:
        arrived(p2[c])
        p2b[c] = ring2(c, order[c][1], line[c])

    def forward(k):
        for c in three:
            arrived(p3[c][k])
            p3b[c][k] = ring2(c, order[c][2], group(c, k))
            for step in (3, 1):
                w = group(c, k)
                w[order[c][2]] = one(nxt(pos[order[c][2]], step))
                share(c, k, w)

    def settle(k):
        for c in three:
            arrived(p3b[c][k])
            w = group(c, k)
            w[order[c][2]] = one(nxt(pos[order[c][2]], 2))
            share(c, k, w)

    def product(s, p, a0, a1, fields):
        left, right = [], []
        for a in range(a0, a1):
            half = [fields(a * 4 + s * 2 + r) for r in range(2)]
            left.append(jnp.concatenate(half, axis=0))
            right.append(P2[s, p * 16 + a].reshape(256, 128))
        return lax.dot_general(
            jnp.concatenate(left, axis=1), jnp.concatenate(right, axis=1),
            (((1,), (1,)), ((), ())), preferred_element_type=F32)

    def contract(c, k, base_off, n_off, copies):
        arrived(copies)
        off, first_place, places = GROUPS[k]
        v = nxt(pos[order[c][1]], off)
        if c == 0:
            def step(i, c2):
                z = nxt(pos["z"], base_off + i // places)
                xx = first_place + lax.rem(i, places)
                got = [product(*part[:1], xx * 2 + z // 2, *part[1:], lambda slab: S[
                    xx, z, v, :, slab].reshape(32, 128)) for part in PARTS[c]]
                for s, value in enumerate(got):
                    acc[s, :, lax.rem(z, 2), v] += value.reshape(2, 32, 256)
                return c2
            lax.fori_loop(0, n_off * places, step, 0, unroll=2)
        elif c == 1:
            ys = pl.ds(first_place, places)
            for i in range(n_off):
                xx = nxt(pos["x"], base_off + i)
                got = [product(*part[:1], xx * 2 + v // 2, *part[1:], lambda slab: S[
                    xx, v, ys, :, slab].reshape(places * 32, 128)) for part in PARTS[c]]
                for s, value in enumerate(got):
                    acc[s, :, lax.rem(v, 2), ys] += value.reshape(2, places, 32, 256)
        else:
            for i in range(n_off):
                y = nxt(pos["y"], base_off + i)
                for half in range(first_place // 2, (first_place + places) // 2):
                    got = [product(*part[:1], v * 2 + half, *part[1:], lambda slab: S[
                        v, 2 * half:2 * half + 2, y, :, slab].reshape(64, 128)) for part in PARTS[c]]
                    for s, value in enumerate(got):
                        acc[s, :, :, y] += value.reshape(2, 2, 32, 256)

    def early(k):
        for c in three:
            contract(c, k, 3, 3, mate_copies[c, k][:3])

    def late(k):
        for c in three:
            contract(c, k, 2, 1, mate_copies[c, k][3:])

    def spread_all(k):
        for c in three:
            spread(c, k)

    forward(0)
    spread_all(1)
    spread_all(2)
    for c in three:
        arrived(p2b[c])
    early(0)
    settle(0)
    late(0)
    forward(1)
    spread_all(3)
    early(1)
    forward(2)
    spread_all(4)
    settle(1)
    early(2)
    forward(3)
    late(1)
    settle(2)
    early(3)
    late(2)
    forward(4)
    settle(3)
    early(4)
    settle(4)
    late(3)
    late(4)

    hot = (partner[...] == lax.broadcasted_iota(jnp.int32, (256, 256), 0)).astype(F32)
    for s in range(2):
        q = acc[s].reshape(512, 256)
        real = q[0:256, 0:128] + q[256:512, 128:256]
        imag = q[0:256, 128:256] - q[256:512, 0:128]
        for r, v in enumerate((real, imag)):
            got = lax.dot_general(v, hot, (((0,), (0,)), ((), ())), precision=lax.Precision.HIGHEST,
                                  preferred_element_type=F32)
            out[s, r] = got * (1.0 / 128.0)
    for copy in pending:
        copy.wait_send()


def body(phi, tau_fwd, tau_bwd, src_times, partner):
    vm = pl.BlockSpec(memory_space=pltpu.VMEM)
    hbm = pl.BlockSpec(memory_space=pl.ANY)
    res = pl.pallas_call(
        kernel,
        out_shape=jax.ShapeDtypeStruct((2, 2, 128, 256), F32),
        in_specs=[pl.BlockSpec(memory_space=pltpu.SMEM), hbm, hbm, hbm, vm],
        out_specs=vm,
        scratch_shapes=[
            pltpu.VMEM((4, 4, 4, 2, 64, 16, 128), BF16),
            pltpu.VMEM((2, 128, 2, 128, 128), BF16),
            pltpu.VMEM((2, 2, 2, 4, 32, 256), F32),
            pltpu.VMEM((2, 16 * ROW, 128), F32),
            pltpu.VMEM((2048, 256), BF16),
            pltpu.VMEM((2, 16, 2, 128, 128), BF16),
            pltpu.VMEM((4, 2, 16, 4, 16, 128), BF16),
            pltpu.VMEM((2, 8, 2, 128, 128), BF16),
            pltpu.VMEM((2, 8, 2, 128, 128), BF16),
            pltpu.VMEM((256, 256), BF16),
            pltpu.VMEM((256, 256), BF16),
            pltpu.VMEM((6, XF, 4, 16, 128), BF16),
            pltpu.VMEM((2, XF, 4, 16, 128), BF16),
            pltpu.VMEM((2, XF, 4, 16, 128), BF16),
            pltpu.VMEM((4, ZF, 4, 16, 128), BF16),
            pltpu.VMEM((XF, 4, 16, 128), BF16),
            pltpu.VMEM((4, ZF, 4, 16, 128), BF16),
            pltpu.VMEM((6, ZH, 4, 16, 128), BF16),
            pltpu.VMEM((2, ZH, 4, 16, 128), BF16),
            pltpu.SemaphoreType.DMA((NSEM,)),
            pltpu.SemaphoreType.DMA((NSEM,)),
            pltpu.SemaphoreType.DMA((2,)),
            pltpu.SemaphoreType.DMA((2,)),
            pltpu.SemaphoreType.DMA((16,)),
        ],
        compiler_params=pltpu.CompilerParams(collective_id=0, has_side_effects=True, vmem_limit_bytes=67043328),
    )(src_times, phi, tau_fwd, tau_bwd, partner.reshape(1, 256))
    return res.reshape(2, 2, 8, 16, 256).transpose(3, 0, 2, 1, 4)


def solution(mesh):
    in_specs = (
        P("op", "tm", None, None, None),
        P(None, "tm", None, None, None),
        P(None, "tm", None, None, None),
        P(),
        P(),
    )
    out_specs = P("op", None, "tm", None, None)
    return jax.shard_map(body, mesh=mesh, in_specs=in_specs, out_specs=out_specs, check_vma=False)
```
